256 devices in a mesh: dp: 32 (over x, z_lo, y), chan: 8 (over z_hi, core).
Axes of the slice: x: 4, y: 4, z: 8 (z_hi: 4, z_lo: 2; z = z_hi * 2 + z_lo), core: 2. Of those that a mesh axis runs over, the one named last changes fastest.
Arguments:
- patches: bfloat16 [256, 256, 1280], P('dp', None, 'chan'), may hold values from -13 to 13
- cotangent: bfloat16 [256, 256, 1280], P('dp', None, 'chan'), may hold values from -33 to 33
- w_token_in: bfloat16 [640, 256], replicated, may hold values from -0.375 to 0.375
- b_token_in: float32 [640], replicated, may hold values from -3 to 3
- w_token_out: bfloat16 [256, 640], replicated, may hold values from -0.25 to 0.25
- layer_norm_gain: float32 [1280], replicated, may hold values from 0.25 to 1.75
- layer_norm_bias: float32 [1280], replicated, may hold values from -3 to 3
Outputs:
- grad_patches: bfloat16 [256, 256, 1280], P('dp', None, 'chan')
- grad_w_in: float32 [640, 256], replicated
- grad_w_out: float32 [256, 640], replicated
- grad_b_in: float32 [640], replicated
- grad_gain: float32 [1280], P('chan')
- grad_shift: float32 [1280], P('chan')
The draws below stay inside these ranges and needn't reach their ends.
All inputs are finite; a program needn't handle non-finite values.
Results may differ from the reference program's by a relative error of at most 0.0065.
Values may be sent and summed in bfloat16 or wider, within the bound.
A program may use at most 64 MiB of HBM per device.

```python
import math
import jax
import jax.numpy as jnp
from jax import lax

CHANNEL_COUNT = 1280
P_SIZE = 256
HID = 640
IMG_DEV = 8
IMAGES = 256
N_DP = 32


def draw_patches(key, part):
    first_term, second_term = jax.random.split(key, 2)
    base = jnp.clip(jax.random.normal(first_term, (IMAGES, P_SIZE, CHANNEL_COUNT), jnp.float32), -4.0, 4.0)
    scale = jnp.exp(jax.random.uniform(second_term, (CHANNEL_COUNT,), jnp.float32, math.log(0.25), math.log(2.5)))
    values = base * scale
    return values.astype(jnp.bfloat16)


def draw_cotangent(key, part):
    first_term, second_term, third = jax.random.split(key, 3)
    base = jnp.clip(jax.random.normal(first_term, (IMAGES, P_SIZE, CHANNEL_COUNT), jnp.float32), -3.5, 3.5)
    shared = 1.5 * jnp.clip(jax.random.normal(third, (IMAGES, P_SIZE, 1), jnp.float32), -2.5, 2.5)
    rising = 3.0 ** (jnp.arange(IMAGES, dtype=jnp.float32) / max(IMAGES - 1, 1))
    channel = jnp.exp(jax.random.uniform(second_term, (CHANNEL_COUNT,), jnp.float32, -math.log(2.0), math.log(2.0)))
    values = (base * channel + shared) * rising[:, None, None]
    return values.astype(jnp.bfloat16)


def scatter_about(stream_key, dims, deviation, reach, held_as=jnp.bfloat16):
    return jnp.clip(deviation * jax.random.normal(stream_key, dims, jnp.float32), -reach, reach).astype(held_as)


def setup_inputs(seed: int = 0) -> dict:
    streams_of = jax.random.split(jax.random.key(seed), 8)
    return {
        "patches": draw_patches(jax.random.fold_in(streams_of[7], 71), 0),
        "cotangent": draw_cotangent(jax.random.fold_in(streams_of[7], 71), 0),
        "w_token_in": scatter_about(streams_of[2], (HID, P_SIZE), P_SIZE ** -0.5, 0.375),
        "b_token_in": scatter_about(streams_of[3], (HID,), 0.5, 3.0, jnp.float32),
        "w_token_out": scatter_about(streams_of[4], (P_SIZE, HID), HID ** -0.5, 0.25),
        "layer_norm_gain": jnp.clip(1.0 + 0.15 * jax.random.normal(streams_of[5], (CHANNEL_COUNT,), jnp.float32), 0.25, 1.75),
        "layer_norm_bias": scatter_about(streams_of[6], (CHANNEL_COUNT,), 0.5, 3.0, jnp.float32),
    }


eps_norm = 1e-05

def block_grads(xb, gb, w_token_in, b_token_in, w_token_out, layer_norm_gain, layer_norm_bias):
    hi = lax.Precision.HIGHEST
    input_float = xb.astype(jnp.float32)
    row_average = lax.optimization_barrier(jnp.sum(input_float, -1)) / CHANNEL_COUNT
    meansq = lax.optimization_barrier(jnp.sum(input_float * input_float, -1)) / CHANNEL_COUNT
    inverse_deviation = lax.rsqrt(meansq - row_average * row_average + eps_norm)
    centered_input = (input_float - row_average[..., None]) * inverse_deviation[..., None]
    normalized_output = (centered_input * layer_norm_gain + layer_norm_bias).astype(jnp.bfloat16)
    normed_f = normalized_output.astype(jnp.float32)
    w_in = w_token_in.astype(jnp.float32)
    w_out = w_token_out.astype(jnp.float32)
    pre = jnp.einsum('kp,bpc->bkc', w_in, normed_f, precision=hi) + b_token_in[None, :, None]
    cdf = 0.5 * (1.0 + jax.scipy.special.erf(pre / math.sqrt(2.0)))
    act = (pre * cdf).astype(jnp.bfloat16).astype(jnp.float32)
    slope = cdf + pre * jnp.exp(-0.5 * pre * pre) / math.sqrt(2.0 * math.pi)
    gradient_float = gb.astype(jnp.float32)
    grad_act = jnp.einsum('pk,bpc->bkc', w_out, gradient_float, precision=hi)
    grad_pre = (grad_act * slope).astype(jnp.bfloat16).astype(jnp.float32)
    gradient_normalized = jnp.einsum('kp,bkc->bpc', w_in, grad_pre, precision=hi).astype(jnp.bfloat16).astype(jnp.float32)
    dw_out = jnp.einsum('bpc,bkc->pk', gradient_float, act, precision=hi)
    dw_in = jnp.einsum('bkc,bpc->kp', grad_pre, normed_f, precision=hi)
    db_in = lax.optimization_barrier(jnp.sum(grad_pre, axis=(0, 2)))
    gain_gradient = lax.optimization_barrier(jnp.sum(gradient_normalized * centered_input, axis=(0, 1)))
    dshift = lax.optimization_barrier(jnp.sum(gradient_normalized, axis=(0, 1)))
    gradient_centered = gradient_normalized * layer_norm_gain
    first_term = lax.optimization_barrier(jnp.sum(gradient_centered, -1)) / CHANNEL_COUNT
    second_term = lax.optimization_barrier(jnp.sum(gradient_centered * centered_input, -1)) / CHANNEL_COUNT
    input_gradient = gradient_float + inverse_deviation[..., None] * (gradient_centered - first_term[..., None] - centered_input * second_term[..., None])
    return (input_gradient.astype(jnp.bfloat16), (dw_in, dw_out, db_in, gain_gradient, dshift))

def reference(patches, cotangent, w_token_in, b_token_in, w_token_out, layer_norm_gain, layer_norm_bias):
    xs = patches.reshape(N_DP, IMG_DEV, P_SIZE, CHANNEL_COUNT)
    gs = cotangent.reshape(N_DP, IMG_DEV, P_SIZE, CHANNEL_COUNT)

    def step(carry, pair):
        input_gradient, parts = block_grads(pair[0], pair[1], w_token_in, b_token_in, w_token_out, layer_norm_gain, layer_norm_bias)
        return (jax.tree.map(lambda a, b: a + b, carry, parts), input_gradient)
    init = (jnp.zeros((HID, P_SIZE), jnp.float32), jnp.zeros((P_SIZE, HID), jnp.float32), jnp.zeros((HID,), jnp.float32), jnp.zeros((CHANNEL_COUNT,), jnp.float32), jnp.zeros((CHANNEL_COUNT,), jnp.float32))
    totals, dxs = lax.scan(step, init, (xs, gs))
    images = float(IMAGES)
    return (dxs.reshape(IMAGES, P_SIZE, CHANNEL_COUNT), totals[0] / images, totals[1] / images, totals[2] / images, totals[3] / images, totals[4] / images)
```

```python
import math

import jax
import jax.numpy as jnp
from jax import lax
from jax.experimental import pallas as pl
from jax.experimental.pallas import tpu as pltpu
from jax.sharding import PartitionSpec as P

CHANNEL_COUNT = 1280
MESH = pl.DeviceIdType.MESH
eps_norm = 1e-05


def from_everyone(shard, axis):
    copies = jnp.broadcast_to(shard, (lax.axis_size(axis), *shard.shape))
    return lax.all_to_all(copies, axis, split_axis=0, concat_axis=0, tiled=True)


def together(arrays, axis):
    ends = [0]
    for a in arrays:
        ends.append(ends[-1] + a.size)
    so_far = from_everyone(jnp.concatenate([a.ravel() for a in arrays]), axis).sum(axis=0)
    return tuple((so_far[b:e].reshape(a.shape) for a, b, e in zip(arrays, ends, ends[1:])))


def remote(src, dst, send, recv, dev):
    return pltpu.make_async_remote_copy(
        src_ref=src, dst_ref=dst, send_sem=send, recv_sem=recv, device_id=dev, device_id_type=MESH
    )


def place():
    dp, ch = lax.axis_index("dp"), lax.axis_index("chan")
    x, zl, y = dp // 8, (dp // 4) % 2, dp % 4
    zh, core = ch // 2, ch % 2
    return x, y, zh * 2 + zl, core


def device(x, y, z, core):
    return (x * 8 + (z % 2) * 4 + y, (z // 2) * 2 + core)


def reduce_kernel(
    g_ref, small_ref, full_ref, sum_ref, r0, s, r1, t, r2, sm1, smt, sm2, sm3, sm4,
    s0, q0, s1, q1, s2, q2, s3, q3, s4, q4, a1, b1, a2, b2, a3, b3,
):
    x, y, z, core = place()
    other = 1 - core
    q = x * 4 + y
    partner = device(x, y, z, other)

    def plane(j):
        xx, yy = (x + j // 4) % 4, (y + j % 4) % 4
        return device(xx, yy, z, core), xx * 4 + yy

    def column(d):
        return device(x, y, (z + d) % 8, core)

    barrier = pltpu.get_barrier_semaphore()
    for dev in [partner] + [plane(j)[0] for j in range(1, 16)] + [column(d) for d in range(1, 8)]:
        pl.semaphore_signal(barrier, inc=1, device_id=dev, device_id_type=MESH)
    pl.semaphore_wait(barrier, 23)

    sends = []
    c0 = remote(g_ref.at[other], r0, s0, q0, partner)
    c0.start()
    for j in range(1, 16):
        c = remote(small_ref, sm1.at[j], a1.at[j], b1, plane(j)[0])
        c.start()
        sends.append(c)
    c0.wait_recv()
    for i in range(16):
        s[i] = (g_ref[core, i].astype(jnp.float32) + r0[i].astype(jnp.float32)).astype(jnp.bfloat16)
    for j in range(1, 16):
        dev, qq = plane(j)
        c = remote(s.at[qq], r1.at[j], s1.at[j], q1, dev)
        c.start()
        sends.append(c)
    pltpu.make_async_copy(sm1.at[pl.ds(1, 15)], sm1.at[pl.ds(1, 15)], b1).wait()
    acc = small_ref[...]
    for j in range(1, 16):
        acc = acc + sm1[j]
    smt[...] = acc
    for d in range(1, 8):
        c = remote(smt, sm2.at[d], a2.at[d], b2, column(d))
        c.start()
        sends.append(c)
    pltpu.make_async_copy(r1.at[pl.ds(1, 15)], r1.at[pl.ds(1, 15)], q1).wait()
    acc = s[q].astype(jnp.float32)
    for j in range(1, 16):
        acc = acc + r1[j].astype(jnp.float32)
    t[...] = acc.astype(jnp.bfloat16)
    for d in range(1, 8):
        c = remote(t, r2.at[d], s2.at[d], q2, column(d))
        c.start()
        sends.append(c)
    pltpu.make_async_copy(sm2.at[pl.ds(1, 7)], sm2.at[pl.ds(1, 7)], b2).wait()
    near = smt[...] + sm2[7 - 6 * (z % 2)]
    acc = smt[...]
    for d in range(1, 8):
        acc = acc + sm2[d]
    sm3[...] = acc
    c = remote(sm3, sm4, a3, b3, partner)
    c.start()
    sends.append(c)
    pltpu.make_async_copy(r2.at[pl.ds(1, 7)], r2.at[pl.ds(1, 7)], q2).wait()
    acc = t[...].astype(jnp.float32)
    for d in range(1, 8):
        acc = acc + r2[d].astype(jnp.float32)
    full_ref[core, q] = acc.astype(jnp.bfloat16)
    arrive = []
    for j in range(1, 16):
        c = remote(full_ref.at[core, q], full_ref.at[core, q], s3.at[j], q3.at[j], plane(j)[0])
        c.start()
        sends.append(c)
    for j in range(0, 16):
        xx, yy = (x + 4 - j // 4) % 4, (y + 4 - j % 4) % 4
        qq = xx * 4 + yy
        if j:
            pltpu.make_async_copy(full_ref.at[core, qq], full_ref.at[core, qq], q3.at[j]).wait()
        c = remote(full_ref.at[core, qq], full_ref.at[core, qq], s4.at[j], q4, partner)
        c.start()
        sends.append(c)
    pltpu.make_async_copy(sm4, sm4, b3).wait()
    row = lax.broadcasted_iota(jnp.int32, (8, 128), 0)
    sum_ref[...] = jnp.where(row < 5, sm3[...] + sm4[...], near)
    pltpu.make_async_copy(full_ref.at[other], full_ref.at[other], q4).wait()
    c0.wait_send()
    for c in sends:
        c.wait_send()


def reduce_all(g, small):
    b16, f32, dma = jnp.bfloat16, jnp.float32, pltpu.SemaphoreType.DMA
    vmem = pl.BlockSpec(memory_space=pltpu.VMEM)
    return pl.pallas_call(
        reduce_kernel,
        out_shape=(jax.ShapeDtypeStruct((2, 16, 16, 640), b16), jax.ShapeDtypeStruct((8, 128), f32)),
        in_specs=[vmem, vmem],
        out_specs=(vmem, vmem),
        scratch_shapes=[
            pltpu.VMEM((16, 16, 640), b16),
            pltpu.VMEM((16, 16, 640), b16),
            pltpu.VMEM((16, 16, 640), b16),
            pltpu.VMEM((16, 640), b16),
            pltpu.VMEM((8, 16, 640), b16),
            pltpu.VMEM((16, 8, 128), f32),
            pltpu.VMEM((8, 128), f32),
            pltpu.VMEM((8, 8, 128), f32),
            pltpu.VMEM((8, 128), f32),
            pltpu.VMEM((8, 128), f32),
            dma, dma, dma((16,)), dma, dma((8,)), dma, dma((16,)), dma((16,)), dma((16,)), dma,
            dma((16,)), dma, dma((8,)), dma, dma, dma,
        ],
        compiler_params=pltpu.CompilerParams(collective_id=0, has_side_effects=True),
    )(g, small)


def shards(
    patches, cotangent, w_token_in, b_token_in, w_token_out, layer_norm_gain, layer_norm_bias
):
    where = lax.axis_index("chan")
    local_width = patches.shape[2]
    images = float(patches.shape[0] * lax.axis_size("dp"))
    input_float = patches.astype(jnp.float32)
    totals = together((jnp.sum(input_float, -1), jnp.sum(input_float * input_float, -1)), "chan")
    row_average = totals[0] / CHANNEL_COUNT
    inverse_deviation = lax.rsqrt(totals[1] / CHANNEL_COUNT - row_average * row_average + eps_norm)
    local_gain = lax.dynamic_slice_in_dim(layer_norm_gain, where * local_width, local_width, 0)
    local_bias = lax.dynamic_slice_in_dim(layer_norm_bias, where * local_width, local_width, 0)
    centered_input = (input_float - row_average[..., None]) * inverse_deviation[..., None]
    normalized_output = (centered_input * local_gain + local_bias).astype(jnp.bfloat16)
    pre = (
        jnp.einsum("kp,bpc->bkc", w_token_in, normalized_output, preferred_element_type=jnp.float32)
        + b_token_in[None, :, None]
    )
    cdf = 0.5 * (1.0 + jax.scipy.special.erf(pre / math.sqrt(2.0)))
    act = (pre * cdf).astype(jnp.bfloat16)
    slope = cdf + pre * jnp.exp(-0.5 * pre * pre) / math.sqrt(2.0 * math.pi)
    grad_act = jnp.einsum("pk,bpc->bkc", w_token_out, cotangent, preferred_element_type=jnp.float32)
    grad_pre = (grad_act * slope).astype(jnp.bfloat16)
    gradient_normalized = jnp.einsum(
        "kp,bkc->bpc", w_token_in, grad_pre, preferred_element_type=jnp.float32
    ).astype(jnp.bfloat16)
    dw_out = jnp.einsum("bpc,bkc->pk", cotangent, act, preferred_element_type=jnp.float32)
    dw_in = jnp.einsum("bkc,bpc->pk", grad_pre, normalized_output, preferred_element_type=jnp.float32)
    db_in = jnp.sum(grad_pre.astype(jnp.float32), axis=(0, 2))
    gradient_block = gradient_normalized.astype(jnp.float32)
    flat = jnp.concatenate(
        [
            db_in,
            jnp.sum(gradient_block * centered_input, axis=(0, 1)),
            jnp.sum(gradient_block, axis=(0, 1)),
            jnp.zeros((64,), jnp.float32),
        ]
    )
    weights = jnp.stack([dw_in, dw_out]).astype(jnp.bfloat16).reshape(2, 16, 16, 640)
    full, sums = reduce_all(weights, flat.reshape(8, 128))
    full = full.reshape(2, 256, 640).astype(jnp.float32) / images
    sums = sums.reshape(-1) / images
    gradient_centered = gradient_block * local_gain
    first, second = together(
        (jnp.sum(gradient_centered, -1), jnp.sum(gradient_centered * centered_input, -1)), "chan"
    )
    first_term = first / CHANNEL_COUNT
    second_term = second / CHANNEL_COUNT
    result = cotangent.astype(jnp.float32) + inverse_deviation[..., None] * (
        gradient_centered - first_term[..., None] - centered_input * second_term[..., None]
    )
    grad_patches = result.astype(jnp.bfloat16)
    return grad_patches, full[0].T, full[1], sums[:640], sums[640:800], sums[800:960]


def solution(mesh):
    placed = (P("dp", None, "chan"), P("dp", None, "chan"), P(), P(), P(), P(), P())
    return jax.shard_map(
        shards,
        mesh=mesh,
        in_specs=placed,
        out_specs=(P("dp", None, "chan"), P(), P(), P(), P("chan"), P("chan")),
        check_vma=False,
    )
```

```python
import math

import jax
import jax.numpy as jnp
from jax import lax
from jax.experimental import pallas as pl
from jax.experimental.pallas import tpu as pltpu
from jax.sharding import PartitionSpec as P

CHANNELS = 1280
PATCH = 256
HID = 640
LOCAL = 160
IMG = 8
WIDE = IMG * LOCAL
IMAGES = 256
MESH = pl.DeviceIdType.MESH
eps_norm = 1e-05
F32, BF16 = jnp.float32, jnp.bfloat16


def remote(src, dst, send, recv, dev):
    return pltpu.make_async_remote_copy(
        src_ref=src, dst_ref=dst, send_sem=send, recv_sem=recv, device_id=dev, device_id_type=MESH
    )


def arrived(ref, sem):
    pltpu.make_async_copy(ref, ref, sem).wait()


def place():
    dp, ch = lax.axis_index("dp"), lax.axis_index("chan")
    x, zl, y = dp // 8, (dp // 4) % 2, dp % 4
    zh, core = ch // 2, ch % 2
    return x, y, zh * 2 + zl, core


def device(x, y, z, core):
    return (x * 8 + (z % 2) * 4 + y, (z // 2) * 2 + core)


def dot(a, b):
    return jnp.dot(a, b, preferred_element_type=F32)


def dot_nt(a, b):
    return lax.dot_general(a, b, (((1,), (1,)), ((), ())), preferred_element_type=F32)


def picks(r, j, which):
    b = ((r >> 3) & 1) * 4 + (r & 3)
    return (((r >> 2) & 1) == which) & (j >= b * LOCAL) & (j < b * LOCAL + LOCAL)


def halves(v):
    hi = v.astype(BF16)
    return hi, (v - hi.astype(F32)).astype(BF16)


def row_totals(stats):
    return jnp.transpose(stats)[:16]


def columns(v):
    hi = v.astype(BF16).astype(F32)
    mid = (v - hi).astype(BF16).astype(F32)
    low = v - hi - mid
    stacked = jnp.concatenate([hi, mid, low, jnp.zeros((80, PATCH), F32)], axis=0)
    return jnp.transpose(stacked).astype(BF16)


def kernel(
    x_hbm, g_hbm, win_hbm, wout_hbm, b_ref, gain_ref, bias_ref,
    out_ref, dwin_ref, dwout_ref, db_ref, norm_ref,
    xv, gv, win, wout, winT, woutT, xc, left, right, ga, xh, rs, gn, bcol, gb, sel, spread,
    e_src, e_in, e_sum, e_far, f_src, f_in, f_sum, f_far,
    grads, r0, s, r1, t, r2, full, small, sm1, smt, sm2, sm3, sm4,
    ld, es, eq1, eq2, fs, fq1, fq2, s0, q0, s1, q1, s2, q2, s3, q3, s4, q4, a1, b1, a2, b2, a3, b3,
):
    x, y, z, core = place()
    other = 1 - core
    q = x * 4 + y
    partner = device(x, y, z, other)
    sends = []

    def start(c):
        c.start()
        sends.append(c)

    def plane(j):
        xx, yy = (x + j // 4) % 4, (y + j % 4) % 4
        return device(xx, yy, z, core), xx * 4 + yy

    def column(d, c=core):
        return device(x, y, (z + d) % 8, c)

    loads = [
        pltpu.make_async_copy(a, b, ld.at[i])
        for i, (a, b) in enumerate(((x_hbm, xv), (g_hbm, gv), (wout_hbm, wout), (win_hbm, win)))
    ]
    for c in loads:
        c.start()

    barrier = pltpu.get_barrier_semaphore()
    peers = [partner] + [plane(j)[0] for j in range(1, 16)] + [column(d) for d in range(1, 8)]
    peers += [column(d, other) for d in (2, 4, 6)]
    for dev in peers:
        pl.semaphore_signal(barrier, inc=1, device_id=dev, device_id_type=MESH)

    j = lax.broadcasted_iota(jnp.int32, (WIDE, 128), 0)
    r = lax.broadcasted_iota(jnp.int32, (WIDE, 128), 1)
    for which in range(2):
        sel[which] = jnp.where((r < 16) & picks(r, j, which), 1.0, 0.0).astype(BF16)
    r = lax.broadcasted_iota(jnp.int32, (128, WIDE), 0)
    j = lax.broadcasted_iota(jnp.int32, (128, WIDE), 1)
    for which in range(2):
        spread[which] = jnp.where((r < 48) & picks(r, j, which), 1.0, 0.0).astype(BF16)

    def total(first, second):
        hi, low = halves(second)
        return first, dot(hi, sel[1]) + dot(low, sel[1])

    loads[0].wait()
    for b in range(IMG):
        xc[:, pl.ds(b * LOCAL, LOCAL)] = xv[b]
    xf = xc[...].astype(F32)
    hi, low = halves(xf * xf)
    e_src[...] = row_totals(dot(xc[...], sel[0]) + dot(hi, sel[1]) + dot(low, sel[1]))
    pl.semaphore_wait(barrier, len(peers))
    start(remote(e_src, e_in, es.at[0], eq1, partner))

    loads[1].wait()
    for b in range(IMG):
        left[1, :, pl.ds(b * LOCAL, LOCAL)] = gv[b]
    loads[2].wait()
    woutT[...] = jnp.transpose(wout[...])

    def second_step(src, came, summed, far, sem1, send, sem2):
        arrived(came, sem1)
        both = src[...] + came[...]
        summed[0] = both[:8]
        summed[1] = both[8:]
        n = 1
        for d in (2, 4, 6):
            for c in (core, other):
                start(remote(summed.at[core], far.at[d // 2 - 1, core], send.at[n], sem2, column(d, c)))
                n += 1

    def finish(summed, far, sem2):
        arrived(far, sem2)
        tot = summed[...] + far[0] + far[1] + far[2]
        return tot * (1.0 / CHANNELS)

    second_step(e_src, e_in, e_sum, e_far, eq1, es, eq2)

    ga[...] = dot(woutT[...], left[1])
    loads[3].wait()
    winT[...] = jnp.transpose(win[...])
    bcol[...] = jnp.transpose(jnp.broadcast_to(b_ref[...], (128, HID)))
    where = z // 2 * 2 + core
    for i, ref in enumerate((gain_ref, bias_ref)):
        mine = ref[pl.ds(where, 1), :]
        for b in range(IMG):
            gb[pl.ds(i, 1), pl.ds(b * LOCAL, LOCAL)] = mine

    mean_sq = finish(e_sum, e_far, eq2)
    rows = []
    for h in range(2):
        mean = mean_sq[h, :4]
        rows += [mean, lax.rsqrt(mean_sq[h, 4:] - mean * mean + eps_norm)]
    cols = columns(jnp.concatenate(rows, axis=0))
    rs[...] = dot(cols, spread[1])
    xhat = (xc[...].astype(F32) - dot(cols, spread[0])) * rs[...]
    xh[...] = xhat
    left[0] = (xhat * gb[0:1, :] + gb[1:2, :]).astype(BF16)

    for k in range(0, HID, 128):
        ks = pl.ds(k, 128)
        pre = dot(win[ks, :], left[0]) + bcol[ks, 0:1]
        cdf = 0.5 * (1.0 + lax.erf(pre * (1.0 / math.sqrt(2.0))))
        right[1, ks, :] = (pre * cdf).astype(BF16)
        slope = cdf + pre * jnp.exp(-0.5 * pre * pre) * (1.0 / math.sqrt(2.0 * math.pi))
        right[0, ks, :] = (ga[ks, :] * slope).astype(BF16)

    grads[other] = dot_nt(left[other], right[other]).astype(BF16).reshape(16, 16, HID)
    start(remote(grads.at[other], r0, s0, q0, partner))
    grads[core] = dot_nt(left[core], right[core]).astype(BF16).reshape(16, 16, HID)
    arrived(r0, q0)
    for i in range(16):
        s[i] = (grads[core, i].astype(F32) + r0[i].astype(F32)).astype(BF16)
    for j in range(1, 16):
        dev, qq = plane(j)
        start(remote(s.at[qq], r1.at[j], s1.at[j], q1, dev))

    gn[...] = dot(winT[...], right[0]).astype(BF16)
    gnf = gn[...].astype(F32)
    along = gnf * xh[...]
    gain = gb[0:1, :]
    hi1, low1 = halves(gnf * gain)
    hi2, low2 = halves(along * gain)
    f_src[...] = row_totals(
        dot(hi1, sel[0]) + dot(low1, sel[0]) + dot(hi2, sel[1]) + dot(low2, sel[1])
    )
    start(remote(f_src, f_in, fs.at[0], fq1, partner))

    db = dot_nt(jnp.ones((8, WIDE), BF16), right[0])[0:1]
    by_channel = [jnp.sum(v, axis=0, keepdims=True) for v in (along, gnf)]
    for i in range(5):
        small[pl.ds(i, 1), :] = db[:, i * 128 : i * 128 + 128]
    for i, v in enumerate(by_channel):
        one = v[:, :LOCAL]
        for b in range(1, IMG):
            one = one + v[:, b * LOCAL : b * LOCAL + LOCAL]
        small[pl.ds(5 + i, 1), :] = one[:, :128]
        small[pl.ds(7, 1), pl.ds(32 * i, 32)] = one[:, 128:]
    small[pl.ds(7, 1), pl.ds(64, 64)] = jnp.zeros((1, 64), F32)
    for j in range(1, 16):
        start(remote(small, sm1.at[j], a1.at[j], b1, plane(j)[0]))

    second_step(f_src, f_in, f_sum, f_far, fq1, fs, fq2)

    arrived(r1.at[pl.ds(1, 15)], q1)
    acc = s[q].astype(F32)
    for j in range(1, 16):
        acc = acc + r1[j].astype(F32)
    t[...] = acc.astype(BF16)
    for d in range(1, 8):
        start(remote(t, r2.at[d], s2.at[d], q2, column(d)))

    means = finish(f_sum, f_far, fq2)
    cols = columns(means.reshape(16, PATCH))
    inner = gn[...].astype(F32) * gb[0:1, :] - dot(cols, spread[0]) - xh[...] * dot(cols, spread[1])
    res = (left[1].astype(F32) + rs[...] * inner).astype(BF16)
    for b in range(IMG):
        out_ref[b] = res[:, b * LOCAL : b * LOCAL + LOCAL]

    arrived(r2.at[pl.ds(1, 7)], q2)
    acc = t[...].astype(F32)
    for d in range(1, 8):
        acc = acc + r2[d].astype(F32)
    full[core, q] = acc.astype(BF16)
    for j in range(1, 16):
        start(remote(full.at[core, q], full.at[core, q], s3.at[j], q3.at[j], plane(j)[0]))
    start(remote(full.at[core, q], full.at[core, q], s4.at[0], q4, partner))

    arrived(sm1.at[pl.ds(1, 15)], b1)
    acc = small[...]
    for j in range(1, 16):
        acc = acc + sm1[j]
    smt[...] = acc
    for d in range(1, 8):
        start(remote(smt, sm2.at[d], a2.at[d], b2, column(d)))

    for j in range(1, 16):
        xx, yy = (x + 4 - j // 4) % 4, (y + 4 - j % 4) % 4
        qq = xx * 4 + yy
        arrived(full.at[core, qq], q3.at[j])
        start(remote(full.at[core, qq], full.at[core, qq], s4.at[j], q4, partner))

    arrived(sm2.at[pl.ds(1, 7)], b2)
    near = smt[...] + sm2[7 - 6 * (z % 2)]
    acc = smt[...]
    for d in range(1, 8):
        acc = acc + sm2[d]
    sm3[...] = acc
    start(remote(sm3, sm4, a3, b3, partner))
    arrived(full.at[other], q4)
    arrived(sm4, b3)
    scale = 1.0 / IMAGES
    dwin_ref[...] = jnp.transpose(full[0].reshape(PATCH, HID).astype(F32) * scale)
    dwout_ref[...] = full[1].reshape(PATCH, HID).astype(F32) * scale
    db = (sm3[...] + sm4[...]) * scale
    for i in range(5):
        db_ref[:, pl.ds(i * 128, 128)] = db[i : i + 1, :]
    near = near * scale
    for i in range(2):
        norm_ref[pl.ds(i, 1), pl.ds(0, 128)] = near[5 + i : 6 + i, :]
        norm_ref[pl.ds(i, 1), pl.ds(128, 32)] = near[7:8, 32 * i : 32 * i + 32]
    for c in sends:
        c.wait_send()


def shards(patches, cotangent, w_in, b_in, w_out, gain, bias):
    dma = pltpu.SemaphoreType.DMA
    vmem = pl.BlockSpec(memory_space=pltpu.VMEM)
    hbm = pl.BlockSpec(memory_space=pltpu.HBM)

    def buf(dtype, *shape):
        return pltpu.VMEM(shape, dtype)

    out, dwin, dwout, db, norm = pl.pallas_call(
        kernel,
        out_shape=(
            jax.ShapeDtypeStruct((IMG, PATCH, LOCAL), BF16),
            jax.ShapeDtypeStruct((HID, PATCH), F32),
            jax.ShapeDtypeStruct((PATCH, HID), F32),
            jax.ShapeDtypeStruct((1, HID), F32),
            jax.ShapeDtypeStruct((2, LOCAL), F32),
        ),
        in_specs=[hbm, hbm, hbm, hbm, vmem, vmem, vmem],
        out_specs=(vmem,) * 5,
        scratch_shapes=[
            buf(BF16, IMG, PATCH, LOCAL),
            buf(BF16, IMG, PATCH, LOCAL),
            buf(BF16, HID, PATCH),
            buf(BF16, PATCH, HID),
            buf(BF16, PATCH, HID),
            buf(BF16, HID, PATCH),
            buf(BF16, PATCH, WIDE),
            buf(BF16, 2, PATCH, WIDE),
            buf(BF16, 2, HID, WIDE),
            buf(F32, HID, WIDE),
            buf(F32, PATCH, WIDE),
            buf(F32, PATCH, WIDE),
            buf(BF16, PATCH, WIDE),
            buf(F32, HID, 128),
            buf(F32, 2, WIDE),
            buf(BF16, 2, WIDE, 128),
            buf(BF16, 2, 128, WIDE),
            buf(F32, 16, PATCH), buf(F32, 16, PATCH), buf(F32, 2, 8, PATCH), buf(F32, 3, 2, 8, PATCH),
            buf(F32, 16, PATCH), buf(F32, 16, PATCH), buf(F32, 2, 8, PATCH), buf(F32, 3, 2, 8, PATCH),
            buf(BF16, 2, 16, 16, HID),
            buf(BF16, 16, 16, HID),
            buf(BF16, 16, 16, HID),
            buf(BF16, 16, 16, HID),
            buf(BF16, 16, HID),
            buf(BF16, 8, 16, HID),
            buf(BF16, 2, 16, 16, HID),
            buf(F32, 8, 128),
            buf(F32, 16, 8, 128),
            buf(F32, 8, 128),
            buf(F32, 8, 8, 128),
            buf(F32, 8, 128),
            buf(F32, 8, 128),
            dma((4,)), dma((7,)), dma, dma, dma((7,)), dma, dma,
            dma, dma, dma((16,)), dma, dma((8,)), dma, dma((16,)), dma((16,)), dma((16,)), dma,
            dma((16,)), dma, dma((8,)), dma, dma, dma,
        ],
        compiler_params=pltpu.CompilerParams(
            collective_id=0, has_side_effects=True, vmem_limit_bytes=48 * 1024 * 1024
        ),
    )(
        patches, cotangent, w_in, w_out,
        b_in.reshape(1, HID), gain.reshape(IMG, LOCAL), bias.reshape(IMG, LOCAL),
    )
    return out, dwin, dwout, db.reshape(HID), norm[0], norm[1]


def solution(mesh):
    placed = (P("dp", None, "chan"), P("dp", None, "chan"), P(), P(), P(), P(), P())
    return jax.shard_map(
        shards,
        mesh=mesh,
        in_specs=placed,
        out_specs=(P("dp", None, "chan"), P(), P(), P(), P("chan"), P("chan")),
        check_vma=False,
    )
```

```python
import math

import jax
import jax.numpy as jnp
from jax import lax
from jax.experimental import pallas as pl
from jax.experimental.pallas import tpu as pltpu
from jax.sharding import PartitionSpec as P

CHANNELS = 1280
PATCH = 256
HID = 640
LOCAL = 160
IMG = 8
ROWS = IMG * LOCAL
IMAGES = 256
MESH = pl.DeviceIdType.MESH
eps_norm = 1e-05
F32, BF16 = jnp.float32, jnp.bfloat16


def remote(src, dst, send, recv, dev):
    return pltpu.make_async_remote_copy(
        src_ref=src, dst_ref=dst, send_sem=send, recv_sem=recv, device_id=dev, device_id_type=MESH
    )


def arrived(ref, sem):
    pltpu.make_async_copy(ref, ref, sem).wait()


def place():
    dp, ch = lax.axis_index("dp"), lax.axis_index("chan")
    x, zl, y = dp // 8, (dp // 4) % 2, dp % 4
    zh, core = ch // 2, ch % 2
    return x, y, zh * 2 + zl, core


def device(x, y, z, core):
    return (x * 8 + (z % 2) * 4 + y, (z // 2) * 2 + core)


def dot(a, b):
    return jnp.dot(a, b, preferred_element_type=F32)


def dot_nt(a, b):
    return lax.dot_general(a, b, (((1,), (1,)), ((), ())), preferred_element_type=F32)


def slot(which, image):
    return image // 4 * 8 + which * 4 + image % 4


def kernel(
    x_hbm, g_hbm, win_hbm, wout_hbm, b_hbm, gain_hbm, bias_hbm,
    out_ref, full, sum_ref,
    xv, win, wout, winT, bv, gv, rows10, left, flip, right, ga, xh, rs, gn, gcol,
    e_src, e_in, e_sum, e_far, f_src, f_in, f_sum, f_far,
    grads, r0, s, r1, t, r2, small, sm1, smt, sm2, sm3, sm4,
    ld, es, eq1, eq2, fs, fq1, fq2, s0, q0, s1, q1, s2, q2, s3, q3, s4, q4, a1, b1, a2, b2, a3, b3,
):
    x, y, z, core = place()
    other = 1 - core
    q = x * 4 + y
    partner = device(x, y, z, other)
    sends = []

    def start(c):
        c.start()
        sends.append(c)

    def plane(j):
        xx, yy = (x + j // 4) % 4, (y + j % 4) % 4
        return device(xx, yy, z, core), xx * 4 + yy

    def column(d, c=core):
        return device(x, y, (z + d) % 8, c)

    def image(b):
        return pl.ds(b * LOCAL, LOCAL)

    loads = [
        pltpu.make_async_copy(a, b, ld.at[i])
        for i, (a, b) in enumerate(
            (
                (x_hbm, xv), (g_hbm, left.at[1]), (wout_hbm, wout), (win_hbm, win),
                (b_hbm, bv), (gain_hbm, gv.at[0]), (bias_hbm, gv.at[1]),
            )
        )
    ]
    for c in loads:
        c.start()

    barrier = pltpu.get_barrier_semaphore()
    peers = [partner] + [plane(j)[0] for j in range(1, 16)] + [column(d) for d in range(1, 8)]
    peers += [column(d, other) for d in (2, 4, 6)]
    for dev in peers:
        pl.semaphore_signal(barrier, inc=1, device_id=dev, device_id_type=MESH)

    loads[0].wait()
    for b in range(IMG):
        v = xv[image(b), :].astype(F32)
        e_src[pl.ds(slot(0, b), 1), :] = jnp.sum(v, axis=0, keepdims=True)
        e_src[pl.ds(slot(1, b), 1), :] = jnp.sum(v * v, axis=0, keepdims=True)
    pl.semaphore_wait(barrier, len(peers))
    start(remote(e_src, e_in, es.at[0], eq1, partner))

    def second_step(src, came, summed, far, sem1, send, sem2):
        arrived(came, sem1)
        both = src[...] + came[...]
        summed[0] = both[:8]
        summed[1] = both[8:]
        n = 1
        for d in (4, 2, 6):
            for c in (core, other):
                start(remote(summed.at[core], far.at[d // 2 - 1, core], send.at[n], sem2, column(d, c)))
                n += 1

    def finish(summed, far, sem2):
        arrived(far, sem2)
        tot = (summed[...] + far[0] + far[1] + far[2]) * (1.0 / CHANNELS)
        return lambda which, b: tot[b // 4, which * 4 + b % 4 : which * 4 + b % 4 + 1, :]

    for c in loads[1:]:
        c.wait()
    where = z // 2 * 2 + core
    for i in range(2):
        rows10[...] = gv[i, 0].reshape(10, 128)
        at = where * 5 // 4
        both = jnp.concatenate([rows10[pl.ds(at, 1), :], rows10[pl.ds(at + 1, 1), :]], axis=1)
        mine = pltpu.roll(both, (256 - where * 5 % 4 * 32) % 256, 1)
        col = jnp.transpose(jnp.broadcast_to(mine, (128, 256)))
        gcol[i] = jnp.broadcast_to(col[:LOCAL, 0:1], (LOCAL, PATCH))
    second_step(e_src, e_in, e_sum, e_far, eq1, es, eq2)
    winT[...] = jnp.transpose(win[...])
    for b in range(IMG):
        ga[image(b), :] = dot(left[1, image(b), :], wout[...])
    flip[1] = jnp.transpose(left[1])

    moment = finish(e_sum, e_far, eq2)
    bias = bv[...].reshape(1, HID)
    for b in range(IMG):
        mean = moment(0, b)
        rstd = lax.rsqrt(moment(1, b) - mean * mean + eps_norm)
        rs[pl.ds(b, 1), :] = rstd
        xhat = (xv[image(b), :].astype(F32) - mean) * rstd
        xh[image(b), :] = xhat
        normed = (xhat * gcol[0] + gcol[1]).astype(BF16)
        left[0, image(b), :] = normed
        pre = dot(normed, winT[...]) + bias
        cdf = 0.5 * (1.0 + lax.erf(pre * (1.0 / math.sqrt(2.0))))
        right[1, image(b), :] = (pre * cdf).astype(BF16)
        slope = cdf + pre * jnp.exp(-0.5 * pre * pre) * (1.0 / math.sqrt(2.0 * math.pi))
        right[0, image(b), :] = (ga[image(b), :] * slope).astype(BF16)
    flip[0] = jnp.transpose(left[0])

    grads[other] = dot(flip[other], right[other]).astype(BF16).reshape(16, 16, HID)
    start(remote(grads.at[other], r0, s0, q0, partner))
    grads[core] = dot(flip[core], right[core]).astype(BF16).reshape(16, 16, HID)
    arrived(r0, q0)
    for i in range(16):
        s[i] = (grads[core, i].astype(F32) + r0[i].astype(F32)).astype(BF16)
    for j in range(1, 16):
        dev, qq = plane(j)
        start(remote(s.at[qq], r1.at[j], s1.at[j], q1, dev))

    by_gain = by_shift = None
    for b in range(IMG):
        v = dot(right[0, image(b), :], win[...]).astype(BF16)
        gn[image(b), :] = v
        v = v.astype(F32)
        along = v * xh[image(b), :]
        f_src[pl.ds(slot(0, b), 1), :] = jnp.sum(v * gcol[0], axis=0, keepdims=True)
        f_src[pl.ds(slot(1, b), 1), :] = jnp.sum(along * gcol[0], axis=0, keepdims=True)
        by_gain = along if b == 0 else by_gain + along
        by_shift = v if b == 0 else by_shift + v
    start(remote(f_src, f_in, fs.at[0], fq1, partner))

    db = dot(jnp.ones((8, ROWS), BF16), right[0])[0:1]
    for i in range(5):
        small[pl.ds(i, 1), :] = db[:, i * 128 : i * 128 + 128]
    ones = jnp.ones((8, PATCH), BF16)
    for i, v in enumerate((by_gain, by_shift)):
        hi = v.astype(BF16)
        rest = v - hi.astype(F32)
        mid = rest.astype(BF16)
        low = (rest - mid.astype(F32)).astype(BF16)
        one = (dot_nt(ones, hi) + dot_nt(ones, mid) + dot_nt(ones, low))[0:1]
        small[pl.ds(5 + i, 1), :] = one[:, :128]
        small[pl.ds(7, 1), pl.ds(32 * i, 32)] = one[:, 128:]
    small[pl.ds(7, 1), pl.ds(64, 64)] = jnp.zeros((1, 64), F32)
    for j in range(1, 16):
        start(remote(small, sm1.at[j], a1.at[j], b1, plane(j)[0]))

    second_step(f_src, f_in, f_sum, f_far, fq1, fs, fq2)

    arrived(r1.at[pl.ds(1, 15)], q1)
    acc = s[q].astype(F32)
    for j in range(1, 16):
        acc = acc + r1[j].astype(F32)
    t[...] = acc.astype(BF16)
    for d in (4, 3, 5, 2, 6, 1, 7):
        start(remote(t, r2.at[d], s2.at[d], q2, column(d)))

    moment = finish(f_sum, f_far, fq2)
    for b in range(IMG):
        inner = gn[image(b), :].astype(F32) * gcol[0] - moment(0, b) - xh[image(b), :] * moment(1, b)
        out_ref[image(b), :] = (left[1, image(b), :].astype(F32) + rs[pl.ds(b, 1), :] * inner).astype(BF16)

    arrived(r2.at[pl.ds(1, 7)], q2)
    acc = t[...].astype(F32)
    for d in range(1, 8):
        acc = acc + r2[d].astype(F32)
    full[core, q] = acc.astype(BF16)
    for j in range(1, 16):
        start(remote(full.at[core, q], full.at[core, q], s3.at[j], q3.at[j], plane(j)[0]))
    start(remote(full.at[core, q], full.at[core, q], s4.at[0], q4, partner))

    arrived(sm1.at[pl.ds(1, 15)], b1)
    acc = small[...]
    for j in range(1, 16):
        acc = acc + sm1[j]
    smt[...] = acc
    for d in range(1, 8):
        start(remote(smt, sm2.at[d], a2.at[d], b2, column(d)))

    for j in range(1, 16):
        xx, yy = (x + 4 - j // 4) % 4, (y + 4 - j % 4) % 4
        qq = xx * 4 + yy
        arrived(full.at[core, qq], q3.at[j])
        start(remote(full.at[core, qq], full.at[core, qq], s4.at[j], q4, partner))

    arrived(sm2.at[pl.ds(1, 7)], b2)
    near = smt[...] + sm2[7 - 6 * (z % 2)]
    acc = smt[...]
    for d in range(1, 8):
        acc = acc + sm2[d]
    sm3[...] = acc
    start(remote(sm3, sm4, a3, b3, partner))
    arrived(sm4, b3)
    row = lax.broadcasted_iota(jnp.int32, (8, 128), 0)
    sum_ref[...] = jnp.where(row < 5, sm3[...] + sm4[...], near) * (1.0 / IMAGES)
    arrived(full.at[other], q4)
    for c in sends:
        c.wait_send()


def last_kernel(d_ref, full, sum_ref, out, dwin, dwout, db, gain, shift, v1, v2, v3, v4, v5, sem):
    copies = []

    def put(i, src, dst):
        c = pltpu.make_async_copy(src, dst, sem.at[i])
        c.start()
        copies.append(c)

    put(0, d_ref, out)
    v2[...] = full[1].reshape(PATCH, HID).astype(F32) * (1.0 / IMAGES)
    put(1, v2, dwout)
    v1[...] = jnp.transpose(full[0].reshape(PATCH, HID).astype(F32)) * (1.0 / IMAGES)
    put(2, v1, dwin)
    v3[...] = sum_ref[0:5, :].reshape(HID)
    put(3, v3, db)
    for i, (v, dst) in enumerate(((v4, gain), (v5, shift))):
        v[pl.ds(0, 128)] = sum_ref[5 + i, :]
        v[pl.ds(128, 32)] = sum_ref[7, 32 * i : 32 * i + 32]
        put(4 + i, v, dst)
    for c in copies:
        c.wait()


def buf(dtype, *shape):
    return pltpu.VMEM(shape, dtype)


def shards(patches, cotangent, w_in, b_in, w_out, gain, bias):
    dma = pltpu.SemaphoreType.DMA
    vmem = pl.BlockSpec(memory_space=pltpu.VMEM)
    hbm = pl.BlockSpec(memory_space=pltpu.HBM)

    def turned(v):
        return v.transpose(0, 2, 1).reshape(ROWS, PATCH)

    d, full, sums = pl.pallas_call(
        kernel,
        out_shape=(
            jax.ShapeDtypeStruct((ROWS, PATCH), BF16),
            jax.ShapeDtypeStruct((2, 16, 16, HID), BF16),
            jax.ShapeDtypeStruct((8, 128), F32),
        ),
        in_specs=[hbm] * 7,
        out_specs=(vmem,) * 3,
        scratch_shapes=[
            buf(BF16, ROWS, PATCH),
            buf(BF16, HID, PATCH),
            buf(BF16, PATCH, HID),
            buf(BF16, PATCH, HID),
            buf(F32, 1, HID),
            buf(F32, 2, 1, CHANNELS),
            buf(F32, 10, 128),
            buf(BF16, 2, ROWS, PATCH),
            buf(BF16, 2, PATCH, ROWS),
            buf(BF16, 2, ROWS, HID),
            buf(F32, ROWS, HID),
            buf(F32, ROWS, PATCH),
            buf(F32, 8, PATCH),
            buf(BF16, ROWS, PATCH),
            buf(F32, 2, LOCAL, PATCH),
            buf(F32, 16, PATCH), buf(F32, 16, PATCH), buf(F32, 2, 8, PATCH), buf(F32, 3, 2, 8, PATCH),
            buf(F32, 16, PATCH), buf(F32, 16, PATCH), buf(F32, 2, 8, PATCH), buf(F32, 3, 2, 8, PATCH),
            buf(BF16, 2, 16, 16, HID),
            buf(BF16, 16, 16, HID),
            buf(BF16, 16, 16, HID),
            buf(BF16, 16, 16, HID),
            buf(BF16, 16, HID),
            buf(BF16, 8, 16, HID),
            buf(F32, 8, 128),
            buf(F32, 16, 8, 128), buf(F32, 8, 128), buf(F32, 8, 8, 128), buf(F32, 8, 128), buf(F32, 8, 128),
            dma((7,)), dma((7,)), dma, dma, dma((7,)), dma, dma,
            dma, dma, dma((16,)), dma, dma((8,)), dma, dma((16,)), dma((16,)), dma((16,)), dma,
            dma((16,)), dma, dma((8,)), dma, dma, dma,
        ],
        compiler_params=pltpu.CompilerParams(collective_id=0, has_side_effects=True),
    )(
        turned(patches), turned(cotangent), w_in, w_out,
        b_in.reshape(1, HID), gain.reshape(1, CHANNELS), bias.reshape(1, CHANNELS),
    )
    out, dwin, dwout, db, dgain, dshift = pl.pallas_call(
        last_kernel,
        out_shape=(
            jax.ShapeDtypeStruct((ROWS, PATCH), BF16),
            jax.ShapeDtypeStruct((HID, PATCH), F32),
            jax.ShapeDtypeStruct((PATCH, HID), F32),
            jax.ShapeDtypeStruct((HID,), F32),
            jax.ShapeDtypeStruct((LOCAL,), F32),
            jax.ShapeDtypeStruct((LOCAL,), F32),
        ),
        in_specs=[vmem] * 3,
        out_specs=(hbm,) * 6,
        scratch_shapes=[
            buf(F32, HID, PATCH), buf(F32, PATCH, HID), buf(F32, HID), buf(F32, LOCAL), buf(F32, LOCAL), dma((6,)),
        ],
    )(d, full, sums)
    return out.reshape(IMG, LOCAL, PATCH).transpose(0, 2, 1), dwin, dwout, db, dgain, dshift


def solution(mesh):
    placed = (P("dp", None, "chan"), P("dp", None, "chan"), P(), P(), P(), P(), P())
    return jax.shard_map(
        shards,
        mesh=mesh,
        in_specs=placed,
        out_specs=(P("dp", None, "chan"), P(), P(), P(), P("chan"), P("chan")),
        check_vma=False,
    )
```

```python
import math

import jax
import jax.numpy as jnp
from jax import lax
from jax.experimental import pallas as pl
from jax.experimental.pallas import tpu as pltpu
from jax.sharding import PartitionSpec as P

CHANNELS = 1280
PATCH = 256
HID = 640
LOCAL = 160
IMG = 8
ROWS = IMG * LOCAL
IMAGES = 256
MESH = pl.DeviceIdType.MESH
PIECES = ((0, 384), (384, 256))
FAR_FIRST = sorted(range(1, 16), key=lambda j: -min(j // 4, 4 - j // 4) - min(j % 4, 4 - j % 4))
Z_FAR_FIRST = (4, 3, 5, 2, 6, 1, 7)
eps_norm = 1e-05
F32, BF16 = jnp.float32, jnp.bfloat16


def remote(src, dst, send, recv, dev):
    return pltpu.make_async_remote_copy(
        src_ref=src, dst_ref=dst, send_sem=send, recv_sem=recv, device_id=dev, device_id_type=MESH
    )


def arrived(ref, sem):
    pltpu.make_async_copy(ref, ref, sem).wait()


def place():
    dp, ch = lax.axis_index("dp"), lax.axis_index("chan")
    x, zl, y = dp // 8, (dp // 4) % 2, dp % 4
    zh, core = ch // 2, ch % 2
    return x, y, zh * 2 + zl, core


def device(x, y, z, core):
    return (x * 8 + (z % 2) * 4 + y, (z // 2) * 2 + core)


def dot(a, b):
    return jnp.dot(a, b, preferred_element_type=F32)


def dot_nt(a, b):
    return lax.dot_general(a, b, (((1,), (1,)), ((), ())), preferred_element_type=F32)


def slot(which, image):
    return image // 4 * 8 + which * 4 + image % 4


def kernel(
    x_hbm, g_hbm, win_hbm, wout_hbm, b_hbm, gain_hbm, bias_hbm,
    out_ref, full_a, full_b, sum_ref,
    xv, win, wout, winT, bv, gain_v, bias_v, rows5, rows10, left, flip, right, ga, xh, rs, gn, gcol,
    e_src, e_in, e_sum, e_far, f_src, f_in, f_sum, f_far,
    small, sm1, smt, sm2, sm3, sm4,
    ld, es, eq1, eq2, fs, fq1, fq2, a1, b1, a2, b2, a3, b3, *travel,
):
    x, y, z, core = place()
    other = 1 - core
    q = x * 4 + y
    partner = device(x, y, z, other)
    sends = []
    fulls = (full_a, full_b)
    travel = (travel[:16], travel[16:])

    def start(c):
        c.start()
        sends.append(c)

    def plane(j):
        xx, yy = (x + j // 4) % 4, (y + j % 4) % 4
        return device(xx, yy, z, core), xx * 4 + yy

    def column(d, c=core):
        return device(x, y, (z + d) % 8, c)

    def image(b):
        return pl.ds(b * LOCAL, LOCAL)

    loads = [
        pltpu.make_async_copy(a, b, ld.at[i])
        for i, (a, b) in enumerate(
            (
                (g_hbm, left.at[1]), (wout_hbm, wout), (win_hbm, win),
                (b_hbm, bv), (gain_hbm, gain_v), (bias_hbm, bias_v),
            )
        )
    ]
    x_loads = [
        pltpu.make_async_copy(x_hbm.at[image(b)], xv.at[image(b)], ld.at[8 + b]) for b in range(IMG)
    ]
    for c in x_loads + loads:
        c.start()

    barrier = pltpu.get_barrier_semaphore()
    peers = [partner] + [plane(j)[0] for j in range(1, 16)] + [column(d) for d in range(1, 8)]
    peers += [column(d, other) for d in (2, 4, 6)]
    for dev in peers:
        pl.semaphore_signal(barrier, inc=1, device_id=dev, device_id_type=MESH)

    for b in range(IMG):
        x_loads[b].wait()
        v = xv[image(b), :].astype(F32)
        e_src[pl.ds(slot(0, b), 1), :] = jnp.sum(v, axis=0, keepdims=True)
        e_src[pl.ds(slot(1, b), 1), :] = jnp.sum(v * v, axis=0, keepdims=True)
    pl.semaphore_wait(barrier, len(peers))
    start(remote(e_src, e_in, es.at[0], eq1, partner))

    def second_step(src, came, summed, far, sem1, send, sem2):
        arrived(came, sem1)
        both = src[...] + came[...]
        summed[0] = both[:8]
        summed[1] = both[8:]
        n = 1
        for d in (4, 2, 6):
            for c in (core, other):
                start(remote(summed.at[core], far.at[d // 2 - 1, core], send.at[n], sem2, column(d, c)))
                n += 1

    def finish(summed, far, sem2):
        arrived(far, sem2)
        tot = (summed[...] + far[0] + far[1] + far[2]) * (1.0 / CHANNELS)
        return lambda which, b: tot[b // 4, which * 4 + b % 4 : which * 4 + b % 4 + 1, :]

    second_step(e_src, e_in, e_sum, e_far, eq1, es, eq2)
    for c in loads:
        c.wait()
    where = z // 2 * 2 + core
    for i in range(2):
        rows10[...] = (gain_v, bias_v)[i][...].reshape(10, 128)
        at = where * 5 // 4
        both = jnp.concatenate([rows10[pl.ds(at, 1), :], rows10[pl.ds(at + 1, 1), :]], axis=1)
        mine = pltpu.roll(both, (256 - where * 5 % 4 * 32) % 256, 1)
        col = jnp.transpose(jnp.broadcast_to(mine, (128, 256)))
        gcol[i] = jnp.broadcast_to(col[:LOCAL, 0:1], (LOCAL, PATCH))
    winT[...] = jnp.transpose(win[...])
    for b in range(IMG):
        ga[image(b), :] = dot(left[1, image(b), :], wout[...])
    flip[1] = jnp.transpose(left[1])

    moment = finish(e_sum, e_far, eq2)
    rows5[...] = bv[...].reshape(5, 128)
    bias = jnp.concatenate([rows5[i : i + 1, :] for i in range(5)], axis=1)
    for b in range(IMG):
        mean = moment(0, b)
        rstd = lax.rsqrt(moment(1, b) - mean * mean + eps_norm)
        rs[pl.ds(b, 1), :] = rstd
        xhat = (xv[image(b), :].astype(F32) - mean) * rstd
        xh[image(b), :] = xhat
        normed = (xhat * gcol[0] + gcol[1]).astype(BF16)
        left[0, image(b), :] = normed
    flip[0] = jnp.transpose(left[0])

    for (at, width), (grads, r0, *_), sem in zip(PIECES, travel, travel):
        ks = pl.ds(at, width)
        for b in range(IMG):
            pre = dot(left[0, image(b), :], winT[:, ks]) + bias[:, at : at + width]
            cdf = 0.5 * (1.0 + lax.erf(pre * (1.0 / math.sqrt(2.0))))
            right[1, image(b), ks] = (pre * cdf).astype(BF16)
            slope = cdf + pre * jnp.exp(-0.5 * pre * pre) * (1.0 / math.sqrt(2.0 * math.pi))
            right[0, image(b), ks] = (ga[image(b), ks] * slope).astype(BF16)
        grads[other] = dot(flip[other], right[other, :, ks]).astype(BF16).reshape(16, 16, width)
        start(remote(grads.at[other], r0, sem[6], sem[7], partner))
        grads[core] = dot(flip[core], right[core, :, ks]).astype(BF16).reshape(16, 16, width)
    for grads, r0, s, r1, t, r2, s0, q0, s1, q1, *_ in travel:
        arrived(r0, q0)
        for i in range(16):
            s[i] = (grads[core, i].astype(F32) + r0[i].astype(F32)).astype(BF16)
        for j in FAR_FIRST:
            dev, qq = plane(j)
            start(remote(s.at[qq], r1.at[j], s1.at[j], q1, dev))

    by_gain = by_shift = None
    for b in range(IMG):
        v = dot(right[0, image(b), :], win[...]).astype(BF16)
        gn[image(b), :] = v
        v = v.astype(F32)
        along = v * xh[image(b), :]
        f_src[pl.ds(slot(0, b), 1), :] = jnp.sum(v * gcol[0], axis=0, keepdims=True)
        f_src[pl.ds(slot(1, b), 1), :] = jnp.sum(along * gcol[0], axis=0, keepdims=True)
        by_gain = along if b == 0 else by_gain + along
        by_shift = v if b == 0 else by_shift + v
    start(remote(f_src, f_in, fs.at[0], fq1, partner))

    db = dot(jnp.ones((8, ROWS), BF16), right[0])[0:1]
    for i in range(5):
        small[pl.ds(i, 1), :] = db[:, i * 128 : i * 128 + 128]
    ones = jnp.ones((8, PATCH), BF16)
    for i, v in enumerate((by_gain, by_shift)):
        hi = v.astype(BF16)
        rest = v - hi.astype(F32)
        mid = rest.astype(BF16)
        low = (rest - mid.astype(F32)).astype(BF16)
        one = (dot_nt(ones, hi) + dot_nt(ones, mid) + dot_nt(ones, low))[0:1]
        small[pl.ds(5 + i, 1), :] = one[:, :128]
        small[pl.ds(7, 1), pl.ds(32 * i, 32)] = one[:, 128:]
    small[pl.ds(7, 1), pl.ds(64, 64)] = jnp.zeros((1, 64), F32)
    for j in range(1, 16):
        start(remote(small, sm1.at[j], a1.at[j], b1, plane(j)[0]))

    second_step(f_src, f_in, f_sum, f_far, fq1, fs, fq2)

    for grads, r0, s, r1, t, r2, s0, q0, s1, q1, s2, q2, *_ in travel:
        arrived(r1.at[pl.ds(1, 15)], q1)
        acc = s[q].astype(F32)
        for j in range(1, 16):
            acc = acc + r1[j].astype(F32)
        t[...] = acc.astype(BF16)
        for d in Z_FAR_FIRST:
            start(remote(t, r2.at[d], s2.at[d], q2, column(d)))

    moment = finish(f_sum, f_far, fq2)
    for b in range(IMG):
        inner = gn[image(b), :].astype(F32) * gcol[0] - moment(0, b) - xh[image(b), :] * moment(1, b)
        out_ref[image(b), :] = (left[1, image(b), :].astype(F32) + rs[pl.ds(b, 1), :] * inner).astype(BF16)

    arrived(sm1.at[pl.ds(1, 15)], b1)
    acc = small[...]
    for j in range(1, 16):
        acc = acc + sm1[j]
    smt[...] = acc
    for d in Z_FAR_FIRST:
        start(remote(smt, sm2.at[d], a2.at[d], b2, column(d)))

    for full, (grads, r0, s, r1, t, r2, s0, q0, s1, q1, s2, q2, s3, q3, s4, q4) in zip(fulls, travel):
        arrived(r2.at[pl.ds(1, 7)], q2)
        acc = t[...].astype(F32)
        for d in range(1, 8):
            acc = acc + r2[d].astype(F32)
        full[core, q] = acc.astype(BF16)
        for j in FAR_FIRST:
            start(remote(full.at[core, q], full.at[core, q], s3.at[j], q3.at[j], plane(j)[0]))
        start(remote(full.at[core, q], full.at[core, q], s4.at[0], q4, partner))

    arrived(sm2.at[pl.ds(1, 7)], b2)
    near = smt[...] + sm2[7 - 6 * (z % 2)]
    acc = smt[...]
    for d in range(1, 8):
        acc = acc + sm2[d]
    sm3[...] = acc
    start(remote(sm3, sm4, a3, b3, partner))
    for full, (*_, q3, s4, q4) in zip(fulls, travel):
        for j in FAR_FIRST[::-1]:
            xx, yy = (x + 4 - j // 4) % 4, (y + 4 - j % 4) % 4
            qq = xx * 4 + yy
            arrived(full.at[core, qq], q3.at[j])
            start(remote(full.at[core, qq], full.at[core, qq], s4.at[j], q4, partner))
    arrived(sm4, b3)
    row = lax.broadcasted_iota(jnp.int32, (8, 128), 0)
    sum_ref[...] = jnp.where(row < 5, sm3[...] + sm4[...], near) * (1.0 / IMAGES)
    for full, (*_, q4) in zip(fulls, travel):
        arrived(full.at[other], q4)
    for c in sends:
        c.wait_send()


def last_kernel(d_ref, full_a, full_b, sum_ref, out, dwin, dwout, db, gain, shift, v1, v2, v3, v4, v5, sem):
    copies = []

    def put(i, src, dst):
        c = pltpu.make_async_copy(src, dst, sem.at[i])
        c.start()
        copies.append(c)

    put(0, d_ref, out)
    for (at, width), full in zip(PIECES, (full_a, full_b)):
        v2[:, pl.ds(at, width)] = full[1].reshape(PATCH, width).astype(F32) * (1.0 / IMAGES)
    put(1, v2, dwout)
    for n, ((at, width), full) in enumerate(zip(PIECES, (full_a, full_b))):
        rows = pl.ds(at, width)
        v1[rows, :] = jnp.transpose(full[0].reshape(PATCH, width).astype(F32)) * (1.0 / IMAGES)
        put(6 + n, v1.at[rows], dwin.at[rows])
    v3[...] = sum_ref[0:5, :].reshape(HID)
    put(3, v3, db)
    for i, (v, dst) in enumerate(((v4, gain), (v5, shift))):
        v[pl.ds(0, 128)] = sum_ref[5 + i, :]
        v[pl.ds(128, 32)] = sum_ref[7, 32 * i : 32 * i + 32]
        put(4 + i, v, dst)
    for c in copies:
        c.wait()


def buf(dtype, *shape):
    return pltpu.VMEM(shape, dtype)


def shards(patches, cotangent, w_in, b_in, w_out, gain, bias):
    dma = pltpu.SemaphoreType.DMA
    vmem = pl.BlockSpec(memory_space=pltpu.VMEM)
    hbm = pl.BlockSpec(memory_space=pltpu.HBM)

    def turned(v):
        return v.transpose(0, 2, 1).reshape(ROWS, PATCH)

    def piece(width):
        return [
            buf(BF16, 2, 16, 16, width),
            buf(BF16, 16, 16, width),
            buf(BF16, 16, 16, width),
            buf(BF16, 16, 16, width),
            buf(BF16, 16, width),
            buf(BF16, 8, 16, width),
            dma, dma, dma((16,)), dma, dma((8,)), dma, dma((16,)), dma((16,)), dma((16,)), dma,
        ]

    d, full_a, full_b, sums = pl.pallas_call(
        kernel,
        out_shape=(
            jax.ShapeDtypeStruct((ROWS, PATCH), BF16),
            *(jax.ShapeDtypeStruct((2, 16, 16, width), BF16) for _, width in PIECES),
            jax.ShapeDtypeStruct((8, 128), F32),
        ),
        in_specs=[hbm] * 7,
        out_specs=(vmem,) * 4,
        scratch_shapes=[
            buf(BF16, ROWS, PATCH),
            buf(BF16, HID, PATCH),
            buf(BF16, PATCH, HID),
            buf(BF16, PATCH, HID),
            buf(F32, HID),
            buf(F32, CHANNELS),
            buf(F32, CHANNELS),
            buf(F32, 5, 128),
            buf(F32, 10, 128),
            buf(BF16, 2, ROWS, PATCH),
            buf(BF16, 2, PATCH, ROWS),
            buf(BF16, 2, ROWS, HID),
            buf(F32, ROWS, HID),
            buf(F32, ROWS, PATCH),
            buf(F32, 8, PATCH),
            buf(BF16, ROWS, PATCH),
            buf(F32, 2, LOCAL, PATCH),
            buf(F32, 16, PATCH), buf(F32, 16, PATCH), buf(F32, 2, 8, PATCH), buf(F32, 3, 2, 8, PATCH),
            buf(F32, 16, PATCH), buf(F32, 16, PATCH), buf(F32, 2, 8, PATCH), buf(F32, 3, 2, 8, PATCH),
            buf(F32, 8, 128),
            buf(F32, 16, 8, 128), buf(F32, 8, 128), buf(F32, 8, 8, 128), buf(F32, 8, 128), buf(F32, 8, 128),
            dma((16,)), dma((7,)), dma, dma, dma((7,)), dma, dma,
            dma((16,)), dma, dma((8,)), dma, dma, dma,
            *piece(PIECES[0][1]), *piece(PIECES[1][1]),
        ],
        compiler_params=pltpu.CompilerParams(collective_id=0, has_side_effects=True, vmem_limit_bytes=40000000),
    )(
        *(
            pltpu.with_memory_space_constraint(v, pltpu.HBM)
            for v in (turned(patches), turned(cotangent), w_in, w_out, b_in, gain, bias)
        )
    )
    out, dwin, dwout, db, dgain, dshift = pl.pallas_call(
        last_kernel,
        out_shape=(
            jax.ShapeDtypeStruct((ROWS, PATCH), BF16),
            jax.ShapeDtypeStruct((HID, PATCH), F32),
            jax.ShapeDtypeStruct((PATCH, HID), F32),
            jax.ShapeDtypeStruct((HID,), F32),
            jax.ShapeDtypeStruct((LOCAL,), F32),
            jax.ShapeDtypeStruct((LOCAL,), F32),
        ),
        in_specs=[vmem] * 4,
        out_specs=(hbm,) * 6,
        scratch_shapes=[
            buf(F32, HID, PATCH), buf(F32, PATCH, HID), buf(F32, HID), buf(F32, LOCAL), buf(F32, LOCAL), dma((8,)),
        ],
        compiler_params=pltpu.CompilerParams(vmem_limit_bytes=8 * 1024 * 1024),
    )(d, full_a, full_b, sums)
    return out.reshape(IMG, LOCAL, PATCH).transpose(0, 2, 1), dwin, dwout, db, dgain, dshift


def solution(mesh):
    placed = (P("dp", None, "chan"), P("dp", None, "chan"), P(), P(), P(), P(), P())
    return jax.shard_map(
        shards,
        mesh=mesh,
        in_specs=placed,
        out_specs=(P("dp", None, "chan"), P(), P(), P(), P("chan"), P("chan")),
        check_vma=False,
    )
```

```python
import math

import jax
import jax.numpy as jnp
from jax import lax
from jax.experimental import pallas as pl
from jax.experimental.pallas import tpu as pltpu
from jax.sharding import PartitionSpec as P

CHANNELS = 1280
PATCH = 256
HID = 640
LOCAL = 160
IMG = 8
ROWS = IMG * LOCAL
IMAGES = 256
MESH = pl.DeviceIdType.MESH
PIECES = ((0, 384, False), (384, 256, True))
PARTS = {False: 16, True: 10}
eps_norm = 1e-05
F32, BF16 = jnp.float32, jnp.bfloat16


def remote(src, dst, send, recv, dev):
    return pltpu.make_async_remote_copy(
        src_ref=src, dst_ref=dst, send_sem=send, recv_sem=recv, device_id=dev, device_id_type=MESH
    )


def arrived(ref, sem):
    pltpu.make_async_copy(ref, ref, sem).wait()


def each(n, body):
    def step(i, carry):
        body(i)
        return carry

    lax.fori_loop(0, n, step, 0)


def div(a, b):
    return lax.div(jnp.int32(a), jnp.int32(b))


def rem(a, b):
    return lax.rem(jnp.int32(a), jnp.int32(b))


def place():
    dp, ch = lax.axis_index("dp"), lax.axis_index("chan")
    x, zl, y = div(dp, 8), rem(div(dp, 4), 2), rem(dp, 4)
    zh, core = div(ch, 2), rem(ch, 2)
    return x, y, zh * 2 + zl, core


def device(x, y, z, core):
    return (x * 8 + rem(z, 2) * 4 + y, div(z, 2) * 2 + core)


def dot(a, b):
    return jnp.dot(a, b, preferred_element_type=F32)


def dot_nt(a, b):
    return lax.dot_general(a, b, (((1,), (1,)), ((), ())), preferred_element_type=F32)


def slot(which, image):
    return image // 4 * 8 + which * 4 + image % 4


def kernel(
    x_hbm, g_hbm, win_hbm, wout_hbm, b_hbm, gain_hbm, bias_hbm,
    out_ref, *refs,
):
    fulls, (sum_ref, *refs) = refs[: len(PIECES)], refs[len(PIECES) :]
    travel = refs[41:]
    (
        xv, win, wout, winT, bv, gain_v, bias_v, rows5, rows10, left, flip, right, ga, xh, rs, gn, gcol,
        e_src, e_far, f_src, f_in, f_sum, f_far,
        small, sm1, smt, sm2, sm3, sm4,
        ld, es, eq, fs, fq1, fq2, a1, b1, a2, b2, a3, b3,
    ) = refs[:41]
    x, y, z, core = place()
    other = 1 - core
    q = x * 4 + y
    partner = device(x, y, z, other)
    sends = []
    pieces = []
    for (at, width, direct), full in zip(PIECES, fulls):
        n = PARTS[direct]
        pieces.append((pl.ds(at, width), direct, full, travel[:n]))
        travel = travel[n:]

    def start(c):
        c.start()
        sends.append(c)

    def plane(j, c=core):
        xx, yy = rem(x + div(j, 4), 4), rem(y + rem(j, 4), 4)
        return device(xx, yy, z, c), xx * 4 + yy

    def column(d, c=core):
        return device(x, y, rem(z + d, 8), c)

    def image(b):
        return pl.ds(b * LOCAL, LOCAL)

    loads = [
        pltpu.make_async_copy(a, b, ld.at[i])
        for i, (a, b) in enumerate(
            (
                (g_hbm, left.at[1]), (wout_hbm, wout), (win_hbm, win),
                (b_hbm, bv), (gain_hbm, gain_v), (bias_hbm, bias_v),
            )
        )
    ]
    def chan_peers():
        return [column(d, c) for d in (4, 2, 6) for c in (core, other)] + [partner]

    def hop(i):
        return 1 + rem(3 + i, 7)

    def offset(i):
        return 1 + rem(9 + i, 15)

    barrier = pltpu.get_barrier_semaphore()

    def greet(dev):
        pl.semaphore_signal(barrier, inc=1, device_id=dev, device_id_type=MESH)

    for dev in chan_peers():
        greet(dev)
    for d in (3, 5, 1, 7):
        greet(column(d))
    each(15, lambda i: greet(plane(offset(i))[0]))

    x_loads = [
        pltpu.make_async_copy(x_hbm.at[image(b)], xv.at[image(b)], ld.at[8 + b]) for b in range(IMG)
    ]
    for c in x_loads + loads:
        c.start()

    for b in range(IMG):
        x_loads[b].wait()
        v = xv[image(b), :].astype(F32)
        e_src[pl.ds(b, 1), :] = jnp.sum(v, axis=0, keepdims=True)
        e_src[pl.ds(8 + b, 1), :] = jnp.sum(v * v, axis=0, keepdims=True)
    pl.semaphore_wait(barrier, 26)
    for n, dev in enumerate(chan_peers()):
        start(remote(e_src, e_far.at[n], es.at[n], eq, dev))

    def second_step(src, came, summed, far, sem1, send, sem2):
        arrived(came, sem1)
        both = src[...] + came[...]
        summed[0] = both[:8]
        summed[1] = both[8:]
        n = 1
        for d in (4, 2, 6):
            for c in (core, other):
                start(remote(summed.at[core], far.at[d // 2 - 1, core], send.at[n], sem2, column(d, c)))
                n += 1

    def finish(summed, far, sem2):
        arrived(far, sem2)
        tot = (summed[...] + far[0] + far[1] + far[2]) * (1.0 / CHANNELS)
        return lambda which, b: tot[b // 4, which * 4 + b % 4 : which * 4 + b % 4 + 1, :]

    for c in loads:
        c.wait()
    where = div(z, 2) * 2 + core
    for i in range(2):
        rows10[...] = (gain_v, bias_v)[i][...].reshape(10, 128)
        at = div(where * 5, 4)
        both = jnp.concatenate([rows10[pl.ds(at, 1), :], rows10[pl.ds(at + 1, 1), :]], axis=1)
        mine = pltpu.roll(both, rem(256 - rem(where * 5, 4) * 32, 256), 1)
        col = jnp.transpose(jnp.broadcast_to(mine, (128, 256)))
        gcol[i] = jnp.broadcast_to(col[:LOCAL, 0:1], (LOCAL, PATCH))
    winT[...] = jnp.transpose(win[...])
    for b in range(IMG):
        ga[image(b), :] = dot(left[1, image(b), :], wout[...])
    flip[1] = jnp.transpose(left[1])

    arrived(e_far, eq)
    tot = e_src[...]
    for n in range(7):
        tot = tot + e_far[n]
    tot = tot * (1.0 / CHANNELS)
    means = tot[:8]
    rs[...] = lax.rsqrt(tot[8:] - means * means + eps_norm)
    rows5[...] = bv[...].reshape(5, 128)
    bias = jnp.concatenate([rows5[i : i + 1, :] for i in range(5)], axis=1)
    for b in range(IMG):
        xhat = (xv[image(b), :].astype(F32) - means[b : b + 1, :]) * rs[pl.ds(b, 1), :]
        xh[image(b), :] = xhat
        normed = (xhat * gcol[0] + gcol[1]).astype(BF16)
        left[0, image(b), :] = normed
    flip[0] = jnp.transpose(left[0])

    def scatter(direct, parts):
        if direct:
            grads, r1, _, _, s1, q1, *_ = parts

            def give(i):
                j = rem(10 + i, 16)
                dev, qq = plane(j, other)
                remote(grads.at[other, qq], r1.at[16 + j], s1, q1, dev).start()

            def give_own(i):
                dev, qq = plane(offset(i))
                remote(grads.at[core, qq], r1.at[offset(i)], s1, q1, dev).start()
                give(i)

            each(15, give_own)
            give(15)
            return
        grads, r0, s, r1, _, _, _, q0, s1, q1, *_ = parts
        arrived(r0, q0)

        def add(i):
            s[i] = (grads[core, i].astype(F32) + r0[i].astype(F32)).astype(BF16)

        each(16, add)

        def give(i):
            dev, qq = plane(offset(i))
            remote(s.at[qq], r1.at[offset(i)], s1, q1, dev).start()

        each(15, give)

    waiting = None
    for (at, width, _), (ks, direct, _, parts) in zip(PIECES, pieces):
        for b in range(IMG):
            pre = dot(left[0, image(b), :], winT[:, ks]) + bias[:, at : at + width]
            cdf = 0.5 * (1.0 + lax.erf(pre * (1.0 / math.sqrt(2.0))))
            right[1, image(b), ks] = (pre * cdf).astype(BF16)
            slope = cdf + pre * jnp.exp(-0.5 * pre * pre) * (1.0 / math.sqrt(2.0 * math.pi))
            right[0, image(b), ks] = (ga[image(b), ks] * slope).astype(BF16)
        if waiting:
            scatter(*waiting)
        grads = parts[0]
        grads[other] = dot(flip[other], right[other, :, ks]).astype(BF16).reshape(16, 16, width)
        if not direct:
            start(remote(grads.at[other], parts[1], parts[6], parts[7], partner))
        grads[core] = dot(flip[core], right[core, :, ks]).astype(BF16).reshape(16, 16, width)
        waiting = direct, parts
    scatter(*waiting)

    by_gain = by_shift = None
    for b in range(IMG):
        v = dot(right[0, image(b), :], win[...]).astype(BF16)
        gn[image(b), :] = v
        v = v.astype(F32)
        along = v * xh[image(b), :]
        f_src[pl.ds(slot(0, b), 1), :] = jnp.sum(v * gcol[0], axis=0, keepdims=True)
        f_src[pl.ds(slot(1, b), 1), :] = jnp.sum(along * gcol[0], axis=0, keepdims=True)
        by_gain = along if b == 0 else by_gain + along
        by_shift = v if b == 0 else by_shift + v
    start(remote(f_src, f_in, fs.at[0], fq1, partner))

    db = dot(jnp.ones((8, ROWS), BF16), right[0])[0:1]
    for i in range(5):
        small[pl.ds(i, 1), :] = db[:, i * 128 : i * 128 + 128]
    ones = jnp.ones((8, PATCH), BF16)
    for i, v in enumerate((by_gain, by_shift)):
        hi = v.astype(BF16)
        rest = v - hi.astype(F32)
        mid = rest.astype(BF16)
        low = (rest - mid.astype(F32)).astype(BF16)
        one = (dot_nt(ones, hi) + dot_nt(ones, mid) + dot_nt(ones, low))[0:1]
        small[pl.ds(5 + i, 1), :] = one[:, :128]
        small[pl.ds(7, 1), pl.ds(32 * i, 32)] = one[:, 128:]
    small[pl.ds(7, 1), pl.ds(64, 64)] = jnp.zeros((1, 64), F32)
    each(15, lambda i: remote(small, sm1.at[offset(i)], a1, b1, plane(offset(i))[0]).start())

    second_step(f_src, f_in, f_sum, f_far, fq1, fs, fq2)

    for _, direct, _, parts in pieces:
        if direct:
            grads, r1, t, r2, _, q1, s2, q2, *_ = parts
            arrived(r1.at[pl.ds(1, 31)], q1)
            acc = grads[core, q].astype(F32)
        else:
            _, _, s, r1, t, r2, _, _, _, q1, s2, q2, *_ = parts
            arrived(r1.at[pl.ds(1, 15)], q1)
            acc = s[q].astype(F32)
        t[...] = lax.fori_loop(1, r1.shape[0], lambda j, a: a + r1[j].astype(F32), acc).astype(BF16)
        each(7, lambda i: remote(t, r2.at[hop(i)], s2, q2, column(hop(i))).start())

    moment = finish(f_sum, f_far, fq2)
    for b in range(IMG):
        inner = gn[image(b), :].astype(F32) * gcol[0] - moment(0, b) - xh[image(b), :] * moment(1, b)
        out_ref[image(b), :] = (left[1, image(b), :].astype(F32) + rs[pl.ds(b, 1), :] * inner).astype(BF16)

    arrived(sm1.at[pl.ds(1, 15)], b1)
    smt[...] = lax.fori_loop(1, 16, lambda j, a: a + sm1[j], small[...])
    each(7, lambda i: remote(smt, sm2.at[hop(i)], a2, b2, column(hop(i))).start())

    for _, direct, full, parts in pieces:
        t, r2, s2, q2, s3, q3 = parts[2:4] + parts[6:] if direct else parts[4:6] + parts[10:14]
        arrived(r2.at[pl.ds(1, 7)], q2)
        acc = lax.fori_loop(1, 8, lambda d, a: a + r2[d].astype(F32), t[...].astype(F32))
        full[core, q] = acc.astype(BF16)
        mine = full.at[core, q]

        def tell(i):
            remote(mine, mine, s3, q3, plane(offset(i))[0]).start()
            if direct:
                remote(mine, mine, s3, q3, plane(offset(i), other)[0]).start()

        each(15, tell)
        if direct:
            remote(mine, mine, s3, q3, partner).start()

    arrived(sm2.at[pl.ds(1, 7)], b2)
    near = smt[...] + sm2[7 - 6 * rem(z, 2)]
    sm3[...] = lax.fori_loop(1, 8, lambda d, a: a + sm2[d], smt[...])
    start(remote(sm3, sm4, a3, b3, partner))
    for _, direct, full, parts in pieces:
        if not direct:
            q3, s4, q4 = parts[13:]
            arrived(full.at[core, pl.ds(1, 15)], q3)
            remote(full.at[core], full.at[core], s4, q4, partner).start()
    arrived(sm4, b3)
    row = lax.broadcasted_iota(jnp.int32, (8, 128), 0)
    sum_ref[...] = jnp.where(row < 5, sm3[...] + sm4[...], near) * (1.0 / IMAGES)
    for _, direct, full, parts in pieces:
        if direct:
            grads, r1, t, r2, s1, q1, s2, q2, s3, q3 = parts
            r1 = r1.at[pl.ds(1, 31)]
            arrived(r1, q3)
            arrived(r1, s3)
        else:
            _, _, _, r1, _, r2, _, _, s1, _, s2, _, s3, _, s4, q4 = parts
            r1 = r1.at[pl.ds(1, 15)]
            arrived(full.at[other], q4)
            arrived(r1, s3)
            arrived(full.at[core], s4)
        arrived(r1, s1)
        arrived(r2.at[pl.ds(1, 7)], s2)
    arrived(sm1.at[pl.ds(1, 15)], a1)
    arrived(sm2.at[pl.ds(1, 7)], a2)
    for c in sends:
        c.wait_send()


def last_kernel(d_ref, *refs):
    fulls, refs = refs[: len(PIECES)], refs[len(PIECES) :]
    sum_ref, out, dwin, dwout, db, gain, shift, v1, v2, v3, v4, v5, sem = refs
    copies = []

    def put(i, src, dst):
        c = pltpu.make_async_copy(src, dst, sem.at[i])
        c.start()
        copies.append(c)

    put(0, d_ref, out)
    for (at, width, _), full in zip(PIECES, fulls):
        v2[:, pl.ds(at, width)] = full[1].reshape(PATCH, width).astype(F32) * (1.0 / IMAGES)
    put(1, v2, dwout)
    for n, ((at, width, _), full) in enumerate(zip(PIECES, fulls)):
        rows = pl.ds(at, width)
        v1[rows, :] = jnp.transpose(full[0].reshape(PATCH, width).astype(F32)) * (1.0 / IMAGES)
        put(6 + n, v1.at[rows], dwin.at[rows])
    v3[...] = sum_ref[0:5, :].reshape(HID)
    put(3, v3, db)
    for i, (v, dst) in enumerate(((v4, gain), (v5, shift))):
        v[pl.ds(0, 128)] = sum_ref[5 + i, :]
        v[pl.ds(128, 32)] = sum_ref[7, 32 * i : 32 * i + 32]
        put(4 + i, v, dst)
    for c in copies:
        c.wait()


def buf(dtype, *shape):
    return pltpu.VMEM(shape, dtype)


def shards(patches, cotangent, w_in, b_in, w_out, gain, bias):
    dma = pltpu.SemaphoreType.DMA
    vmem = pl.BlockSpec(memory_space=pltpu.VMEM)
    hbm = pl.BlockSpec(memory_space=pltpu.HBM)

    def turned(v):
        return v.transpose(0, 2, 1).reshape(ROWS, PATCH)

    def piece(width, direct):
        halves = [buf(BF16, 16, 16, width), buf(BF16, 16, 16, width)]
        return [
            buf(BF16, 2, 16, 16, width),
            *([] if direct else halves),
            buf(BF16, 32 if direct else 16, 16, width),
            buf(BF16, 16, width),
            buf(BF16, 8, 16, width),
            *[dma] * (6 if direct else 10),
        ]

    d, *fulls, sums = pl.pallas_call(
        kernel,
        out_shape=(
            jax.ShapeDtypeStruct((ROWS, PATCH), BF16),
            *(jax.ShapeDtypeStruct((2, 16, 16, width), BF16) for _, width, _ in PIECES),
            jax.ShapeDtypeStruct((8, 128), F32),
        ),
        in_specs=[hbm] * 7,
        out_specs=(vmem,) * (2 + len(PIECES)),
        scratch_shapes=[
            buf(BF16, ROWS, PATCH),
            buf(BF16, HID, PATCH),
            buf(BF16, PATCH, HID),
            buf(BF16, PATCH, HID),
            buf(F32, HID),
            buf(F32, CHANNELS),
            buf(F32, CHANNELS),
            buf(F32, 5, 128),
            buf(F32, 10, 128),
            buf(BF16, 2, ROWS, PATCH),
            buf(BF16, 2, PATCH, ROWS),
            buf(BF16, 2, ROWS, HID),
            buf(F32, ROWS, HID),
            buf(F32, ROWS, PATCH),
            buf(F32, 8, PATCH),
            buf(BF16, ROWS, PATCH),
            buf(F32, 2, LOCAL, PATCH),
            buf(F32, 16, PATCH), buf(F32, 7, 16, PATCH),
            buf(F32, 16, PATCH), buf(F32, 16, PATCH), buf(F32, 2, 8, PATCH), buf(F32, 3, 2, 8, PATCH),
            buf(F32, 8, 128),
            buf(F32, 16, 8, 128), buf(F32, 8, 128), buf(F32, 8, 8, 128), buf(F32, 8, 128), buf(F32, 8, 128),
            dma((16,)), dma((7,)), dma, dma((7,)), dma, dma,
            dma, dma, dma, dma, dma, dma,
            *(v for _, width, direct in PIECES for v in piece(width, direct)),
        ],
        compiler_params=pltpu.CompilerParams(collective_id=0, has_side_effects=True, vmem_limit_bytes=40000000),
    )(
        *(
            pltpu.with_memory_space_constraint(v, pltpu.HBM)
            for v in (turned(patches), turned(cotangent), w_in, w_out, b_in, gain, bias)
        )
    )
    out, dwin, dwout, db, dgain, dshift = pl.pallas_call(
        last_kernel,
        out_shape=(
            jax.ShapeDtypeStruct((ROWS, PATCH), BF16),
            jax.ShapeDtypeStruct((HID, PATCH), F32),
            jax.ShapeDtypeStruct((PATCH, HID), F32),
            jax.ShapeDtypeStruct((HID,), F32),
            jax.ShapeDtypeStruct((LOCAL,), F32),
            jax.ShapeDtypeStruct((LOCAL,), F32),
        ),
        in_specs=[vmem] * (2 + len(PIECES)),
        out_specs=(hbm,) * 6,
        scratch_shapes=[
            buf(F32, HID, PATCH), buf(F32, PATCH, HID), buf(F32, HID), buf(F32, LOCAL), buf(F32, LOCAL), dma((6 + len(PIECES),)),
        ],
        compiler_params=pltpu.CompilerParams(vmem_limit_bytes=8 * 1024 * 1024),
    )(d, *fulls, sums)
    return out.reshape(IMG, LOCAL, PATCH).transpose(0, 2, 1), dwin, dwout, db, dgain, dshift


def solution(mesh):
    placed = (P("dp", None, "chan"), P("dp", None, "chan"), P(), P(), P(), P(), P())
    return jax.shard_map(
        shards,
        mesh=mesh,
        in_specs=placed,
        out_specs=(P("dp", None, "chan"), P(), P(), P(), P("chan"), P("chan")),
        check_vma=False,
    )
```

```python
import math

import jax
import jax.numpy as jnp
from jax import lax
from jax.experimental import pallas as pl
from jax.experimental.pallas import tpu as pltpu
from jax.sharding import PartitionSpec as P

CHANNELS = 1280
PATCH = 256
HID = 640
LOCAL = 160
IMG = 8
ROWS = IMG * LOCAL
IMAGES = 256
MESH = pl.DeviceIdType.MESH
PIECES = ((0, 384, False), (384, 256, True))
PARTS = {False: 16, True: 10}
eps_norm = 1e-05
F32, BF16 = jnp.float32, jnp.bfloat16


def remote(src, dst, send, recv, dev):
    return pltpu.make_async_remote_copy(
        src_ref=src, dst_ref=dst, send_sem=send, recv_sem=recv, device_id=dev, device_id_type=MESH
    )


def arrived(ref, sem):
    pltpu.make_async_copy(ref, ref, sem).wait()


def each(n, body):
    def step(i, carry):
        body(i)
        return carry

    lax.fori_loop(0, n, step, 0)


def div(a, b):
    return lax.div(jnp.int32(a), jnp.int32(b))


def rem(a, b):
    return lax.rem(jnp.int32(a), jnp.int32(b))


def place():
    dp, ch = lax.axis_index("dp"), lax.axis_index("chan")
    x, zl, y = div(dp, 8), rem(div(dp, 4), 2), rem(dp, 4)
    zh, core = div(ch, 2), rem(ch, 2)
    return x, y, zh * 2 + zl, core


def device(x, y, z, core):
    return (x * 8 + rem(z, 2) * 4 + y, div(z, 2) * 2 + core)


def dot(a, b):
    return jnp.dot(a, b, preferred_element_type=F32)


def dot_nt(a, b):
    return lax.dot_general(a, b, (((1,), (1,)), ((), ())), preferred_element_type=F32)


def slot(which, image):
    return image // 4 * 8 + which * 4 + image % 4


def kernel(
    x_hbm, g_hbm, win_hbm, wout_hbm, b_hbm, gain_hbm, bias_hbm,
    out_ref, *refs,
):
    fulls, (sum_ref, *refs) = refs[: len(PIECES)], refs[len(PIECES) :]
    travel = refs[41:]
    (
        xv, win, wout, winT, bv, gain_v, bias_v, rows5, rows10, left, flip, right, ga, xh, rs, gn, gcol,
        e_src, e_far, f_src, f_in, f_sum, f_far,
        small, sm1, smt, sm2, sm3, sm4,
        ld, es, eq, fs, fq1, fq2, a1, b1, a2, b2, a3, b3,
    ) = refs[:41]
    x, y, z, core = place()
    other = 1 - core
    q = x * 4 + y
    partner = device(x, y, z, other)
    sends = []
    pieces = []
    for (at, width, direct), full in zip(PIECES, fulls):
        n = PARTS[direct]
        pieces.append((pl.ds(at, width), direct, full, travel[:n]))
        travel = travel[n:]

    def start(c):
        c.start()
        sends.append(c)

    def plane(j, c=core):
        xx, yy = rem(x + div(j, 4), 4), rem(y + rem(j, 4), 4)
        return device(xx, yy, z, c), xx * 4 + yy

    def column(d, c=core):
        return device(x, y, rem(z + d, 8), c)

    def image(b):
        return pl.ds(b * LOCAL, LOCAL)

    loads = [
        pltpu.make_async_copy(a, b, ld.at[i])
        for i, (a, b) in enumerate(
            (
                (g_hbm, left.at[1]), (wout_hbm, wout), (win_hbm, win),
                (b_hbm, bv), (gain_hbm, gain_v), (bias_hbm, bias_v),
            )
        )
    ]
    def chan_peers():
        return [column(d, c) for d in (4, 2, 6) for c in (core, other)] + [partner]

    def hop(i):
        return 1 + rem(3 + i, 7)

    def offset(i):
        return 1 + rem(9 + i, 15)

    barrier = pltpu.get_barrier_semaphore()

    def greet(dev):
        pl.semaphore_signal(barrier, inc=1, device_id=dev, device_id_type=MESH)

    for dev in chan_peers():
        greet(dev)
    for d in (3, 5, 1, 7):
        greet(column(d))
    each(15, lambda i: greet(plane(offset(i))[0]))

    x_loads = [
        pltpu.make_async_copy(x_hbm.at[image(b)], xv.at[image(b)], ld.at[8 + b]) for b in range(IMG)
    ]
    for c in x_loads + loads:
        c.start()

    for b in range(IMG):
        x_loads[b].wait()
        v = xv[image(b), :].astype(F32)
        e_src[b // 4, pl.ds(b % 4, 1), :] = jnp.sum(v, axis=0, keepdims=True)
        e_src[b // 4, pl.ds(4 + b % 4, 1), :] = jnp.sum(v * v, axis=0, keepdims=True)
    pl.semaphore_wait(barrier, 26)
    for h in range(2):
        for n, dev in enumerate(chan_peers()):
            start(remote(e_src.at[h], e_far.at[h, n], es.at[7 * h + n], eq.at[h], dev))

    def second_step(src, came, summed, far, sem1, send, sem2):
        arrived(came, sem1)
        both = src[...] + came[...]
        summed[0] = both[:8]
        summed[1] = both[8:]
        n = 1
        for d in (4, 2, 6):
            for c in (core, other):
                start(remote(summed.at[core], far.at[d // 2 - 1, core], send.at[n], sem2, column(d, c)))
                n += 1

    def finish(summed, far, sem2):
        arrived(far, sem2)
        tot = (summed[...] + far[0] + far[1] + far[2]) * (1.0 / CHANNELS)
        return lambda which, b: tot[b // 4, which * 4 + b % 4 : which * 4 + b % 4 + 1, :]

    for c in loads:
        c.wait()
    where = div(z, 2) * 2 + core
    for i in range(2):
        rows10[...] = (gain_v, bias_v)[i][...].reshape(10, 128)
        at = div(where * 5, 4)
        both = jnp.concatenate([rows10[pl.ds(at, 1), :], rows10[pl.ds(at + 1, 1), :]], axis=1)
        mine = pltpu.roll(both, rem(256 - rem(where * 5, 4) * 32, 256), 1)
        col = jnp.transpose(jnp.broadcast_to(mine, (128, 256)))
        gcol[i] = jnp.broadcast_to(col[:LOCAL, 0:1], (LOCAL, PATCH))
    winT[...] = jnp.transpose(win[...])
    for b in range(IMG):
        ga[image(b), :] = dot(left[1, image(b), :], wout[...])
    flip[1] = jnp.transpose(left[1])

    rows5[...] = bv[...].reshape(5, 128)
    bias = jnp.concatenate([rows5[i : i + 1, :] for i in range(5)], axis=1)

    def hidden(b, at, width):
        ks = pl.ds(at, width)
        pre = dot(left[0, image(b), :], winT[:, ks]) + bias[:, at : at + width]
        cdf = 0.5 * (1.0 + lax.erf(pre * (1.0 / math.sqrt(2.0))))
        right[1, image(b), ks] = (pre * cdf).astype(BF16)
        slope = cdf + pre * jnp.exp(-0.5 * pre * pre) * (1.0 / math.sqrt(2.0 * math.pi))
        right[0, image(b), ks] = (ga[image(b), ks] * slope).astype(BF16)

    for h in range(2):
        arrived(e_far.at[h], eq.at[h])
        tot = e_src[h]
        for n in range(7):
            tot = tot + e_far[h, n]
        tot = tot * (1.0 / CHANNELS)
        means = tot[:4]
        rstd = lax.rsqrt(tot[4:] - means * means + eps_norm)
        rs[pl.ds(4 * h, 4), :] = rstd
        for i in range(4):
            b = 4 * h + i
            xhat = (xv[image(b), :].astype(F32) - means[i : i + 1, :]) * rstd[i : i + 1, :]
            xh[image(b), :] = xhat
            left[0, image(b), :] = (xhat * gcol[0] + gcol[1]).astype(BF16)
            hidden(b, *PIECES[0][:2])
    flip[0] = jnp.transpose(left[0])

    def scatter(direct, parts):
        if direct:
            grads, r1, _, _, s1, q1, *_ = parts

            def give(i):
                j = rem(10 + i, 16)
                dev, qq = plane(j, other)
                remote(grads.at[other, qq], r1.at[16 + j], s1, q1, dev).start()

            def give_own(i):
                dev, qq = plane(offset(i))
                remote(grads.at[core, qq], r1.at[offset(i)], s1, q1, dev).start()
                give(i)

            each(15, give_own)
            give(15)
            return
        grads, r0, s, r1, _, _, _, q0, s1, q1, *_ = parts
        arrived(r0, q0)

        def add(i):
            s[i] = (grads[core, i].astype(F32) + r0[i].astype(F32)).astype(BF16)

        each(16, add)

        def give(i):
            dev, qq = plane(offset(i))
            remote(s.at[qq], r1.at[offset(i)], s1, q1, dev).start()

        each(15, give)

    waiting = None
    for (at, width, _), (ks, direct, _, parts) in zip(PIECES, pieces):
        if at:
            for b in range(IMG):
                hidden(b, at, width)
        if waiting:
            scatter(*waiting)
        grads = parts[0]
        grads[other] = dot(flip[other], right[other, :, ks]).astype(BF16).reshape(16, 16, width)
        if not direct:
            start(remote(grads.at[other], parts[1], parts[6], parts[7], partner))
        grads[core] = dot(flip[core], right[core, :, ks]).astype(BF16).reshape(16, 16, width)
        waiting = direct, parts
    scatter(*waiting)

    by_gain = by_shift = None
    for b in range(IMG):
        v = dot(right[0, image(b), :], win[...]).astype(BF16)
        gn[image(b), :] = v
        v = v.astype(F32)
        along = v * xh[image(b), :]
        f_src[pl.ds(slot(0, b), 1), :] = jnp.sum(v * gcol[0], axis=0, keepdims=True)
        f_src[pl.ds(slot(1, b), 1), :] = jnp.sum(along * gcol[0], axis=0, keepdims=True)
        by_gain = along if b == 0 else by_gain + along
        by_shift = v if b == 0 else by_shift + v
    start(remote(f_src, f_in, fs.at[0], fq1, partner))

    db = dot(jnp.ones((8, ROWS), BF16), right[0])[0:1]
    for i in range(5):
        small[pl.ds(i, 1), :] = db[:, i * 128 : i * 128 + 128]
    ones = jnp.ones((8, PATCH), BF16)
    for i, v in enumerate((by_gain, by_shift)):
        hi = v.astype(BF16)
        rest = v - hi.astype(F32)
        mid = rest.astype(BF16)
        low = (rest - mid.astype(F32)).astype(BF16)
        one = (dot_nt(ones, hi) + dot_nt(ones, mid) + dot_nt(ones, low))[0:1]
        small[pl.ds(5 + i, 1), :] = one[:, :128]
        small[pl.ds(7, 1), pl.ds(32 * i, 32)] = one[:, 128:]
    small[pl.ds(7, 1), pl.ds(64, 64)] = jnp.zeros((1, 64), F32)
    each(15, lambda i: remote(small, sm1.at[offset(i)], a1, b1, plane(offset(i))[0]).start())

    second_step(f_src, f_in, f_sum, f_far, fq1, fs, fq2)

    for _, direct, _, parts in pieces:
        if direct:
            grads, r1, t, r2, _, q1, s2, q2, *_ = parts
            arrived(r1.at[pl.ds(1, 31)], q1)
            acc = grads[core, q].astype(F32)
        else:
            _, _, s, r1, t, r2, _, _, _, q1, s2, q2, *_ = parts
            arrived(r1.at[pl.ds(1, 15)], q1)
            acc = s[q].astype(F32)
        t[...] = lax.fori_loop(1, r1.shape[0], lambda j, a: a + r1[j].astype(F32), acc, unroll=r1.shape[0] - 1).astype(BF16)
        each(7, lambda i: remote(t, r2.at[hop(i)], s2, q2, column(hop(i))).start())

    moment = finish(f_sum, f_far, fq2)
    for b in range(IMG):
        inner = gn[image(b), :].astype(F32) * gcol[0] - moment(0, b) - xh[image(b), :] * moment(1, b)
        out_ref[image(b), :] = (left[1, image(b), :].astype(F32) + rs[pl.ds(b, 1), :] * inner).astype(BF16)

    arrived(sm1.at[pl.ds(1, 15)], b1)
    smt[...] = lax.fori_loop(1, 16, lambda j, a: a + sm1[j], small[...])
    each(7, lambda i: remote(smt, sm2.at[hop(i)], a2, b2, column(hop(i))).start())

    for _, direct, full, parts in pieces:
        t, r2, s2, q2, s3, q3 = parts[2:4] + parts[6:] if direct else parts[4:6] + parts[10:14]
        arrived(r2.at[pl.ds(1, 7)], q2)
        acc = lax.fori_loop(1, 8, lambda d, a: a + r2[d].astype(F32), t[...].astype(F32), unroll=7)
        full[core, q] = acc.astype(BF16)
        mine = full.at[core, q]

        def tell(i):
            remote(mine, mine, s3, q3, plane(offset(i))[0]).start()
            if direct:
                remote(mine, mine, s3, q3, plane(offset(i), other)[0]).start()

        each(15, tell)
        if direct:
            remote(mine, mine, s3, q3, partner).start()

    arrived(sm2.at[pl.ds(1, 7)], b2)
    near = smt[...] + sm2[7 - 6 * rem(z, 2)]
    sm3[...] = lax.fori_loop(1, 8, lambda d, a: a + sm2[d], smt[...])
    start(remote(sm3, sm4, a3, b3, partner))
    for _, direct, full, parts in pieces:
        if not direct:
            q3, s4, q4 = parts[13:]
            arrived(full.at[core, pl.ds(1, 15)], q3)
            remote(full.at[core], full.at[core], s4, q4, partner).start()
    arrived(sm4, b3)
    row = lax.broadcasted_iota(jnp.int32, (8, 128), 0)
    sum_ref[...] = jnp.where(row < 5, sm3[...] + sm4[...], near) * (1.0 / IMAGES)
    for _, direct, full, parts in pieces:
        if direct:
            grads, r1, t, r2, s1, q1, s2, q2, s3, q3 = parts
            r1 = r1.at[pl.ds(1, 31)]
            arrived(r1, q3)
            arrived(r1, s3)
        else:
            _, _, _, r1, _, r2, _, _, s1, _, s2, _, s3, _, s4, q4 = parts
            r1 = r1.at[pl.ds(1, 15)]
            arrived(full.at[other], q4)
            arrived(r1, s3)
            arrived(full.at[core], s4)
        arrived(r1, s1)
        arrived(r2.at[pl.ds(1, 7)], s2)
    arrived(sm1.at[pl.ds(1, 15)], a1)
    arrived(sm2.at[pl.ds(1, 7)], a2)
    for c in sends:
        c.wait_send()


def last_kernel(d_ref, *refs):
    fulls, refs = refs[: len(PIECES)], refs[len(PIECES) :]
    sum_ref, out, dwin, dwout, db, gain, shift, v1, v2, v3, v4, v5, sem = refs
    copies = []

    def put(i, src, dst):
        c = pltpu.make_async_copy(src, dst, sem.at[i])
        c.start()
        copies.append(c)

    put(0, d_ref, out)
    for (at, width, _), full in zip(PIECES, fulls):
        v2[:, pl.ds(at, width)] = full[1].reshape(PATCH, width).astype(F32) * (1.0 / IMAGES)
    put(1, v2, dwout)
    for n, ((at, width, _), full) in enumerate(zip(PIECES, fulls)):
        rows = pl.ds(at, width)
        v1[rows, :] = jnp.transpose(full[0].reshape(PATCH, width).astype(F32)) * (1.0 / IMAGES)
        put(6 + n, v1.at[rows], dwin.at[rows])
    v3[...] = sum_ref[0:5, :].reshape(HID)
    put(3, v3, db)
    for i, (v, dst) in enumerate(((v4, gain), (v5, shift))):
        v[pl.ds(0, 128)] = sum_ref[5 + i, :]
        v[pl.ds(128, 32)] = sum_ref[7, 32 * i : 32 * i + 32]
        put(4 + i, v, dst)
    for c in copies:
        c.wait()


def buf(dtype, *shape):
    return pltpu.VMEM(shape, dtype)


def shards(patches, cotangent, w_in, b_in, w_out, gain, bias):
    dma = pltpu.SemaphoreType.DMA
    vmem = pl.BlockSpec(memory_space=pltpu.VMEM)
    hbm = pl.BlockSpec(memory_space=pltpu.HBM)

    def turned(v):
        return v.transpose(0, 2, 1).reshape(ROWS, PATCH)

    def piece(width, direct):
        halves = [buf(BF16, 16, 16, width), buf(BF16, 16, 16, width)]
        return [
            buf(BF16, 2, 16, 16, width),
            *([] if direct else halves),
            buf(BF16, 32 if direct else 16, 16, width),
            buf(BF16, 16, width),
            buf(BF16, 8, 16, width),
            *[dma] * (6 if direct else 10),
        ]

    d, *fulls, sums = pl.pallas_call(
        kernel,
        out_shape=(
            jax.ShapeDtypeStruct((ROWS, PATCH), BF16),
            *(jax.ShapeDtypeStruct((2, 16, 16, width), BF16) for _, width, _ in PIECES),
            jax.ShapeDtypeStruct((8, 128), F32),
        ),
        in_specs=[hbm] * 7,
        out_specs=(vmem,) * (2 + len(PIECES)),
        scratch_shapes=[
            buf(BF16, ROWS, PATCH),
            buf(BF16, HID, PATCH),
            buf(BF16, PATCH, HID),
            buf(BF16, PATCH, HID),
            buf(F32, HID),
            buf(F32, CHANNELS),
            buf(F32, CHANNELS),
            buf(F32, 5, 128),
            buf(F32, 10, 128),
            buf(BF16, 2, ROWS, PATCH),
            buf(BF16, 2, PATCH, ROWS),
            buf(BF16, 2, ROWS, HID),
            buf(F32, ROWS, HID),
            buf(F32, ROWS, PATCH),
            buf(F32, 8, PATCH),
            buf(BF16, ROWS, PATCH),
            buf(F32, 2, LOCAL, PATCH),
            buf(F32, 2, 8, PATCH), buf(F32, 2, 7, 8, PATCH),
            buf(F32, 16, PATCH), buf(F32, 16, PATCH), buf(F32, 2, 8, PATCH), buf(F32, 3, 2, 8, PATCH),
            buf(F32, 8, 128),
            buf(F32, 16, 8, 128), buf(F32, 8, 128), buf(F32, 8, 8, 128), buf(F32, 8, 128), buf(F32, 8, 128),
            dma((16,)), dma((14,)), dma((2,)), dma((7,)), dma, dma,
            dma, dma, dma, dma, dma, dma,
            *(v for _, width, direct in PIECES for v in piece(width, direct)),
        ],
        compiler_params=pltpu.CompilerParams(collective_id=0, has_side_effects=True, vmem_limit_bytes=40000000),
    )(
        *(
            pltpu.with_memory_space_constraint(v, pltpu.HBM)
            for v in (turned(patches), turned(cotangent), w_in, w_out, b_in, gain, bias)
        )
    )
    out, dwin, dwout, db, dgain, dshift = pl.pallas_call(
        last_kernel,
        out_shape=(
            jax.ShapeDtypeStruct((ROWS, PATCH), BF16),
            jax.ShapeDtypeStruct((HID, PATCH), F32),
            jax.ShapeDtypeStruct((PATCH, HID), F32),
            jax.ShapeDtypeStruct((HID,), F32),
            jax.ShapeDtypeStruct((LOCAL,), F32),
            jax.ShapeDtypeStruct((LOCAL,), F32),
        ),
        in_specs=[vmem] * (2 + len(PIECES)),
        out_specs=(hbm,) * 6,
        scratch_shapes=[
            buf(F32, HID, PATCH), buf(F32, PATCH, HID), buf(F32, HID), buf(F32, LOCAL), buf(F32, LOCAL), dma((6 + len(PIECES),)),
        ],
        compiler_params=pltpu.CompilerParams(vmem_limit_bytes=8 * 1024 * 1024),
    )(d, *fulls, sums)
    return out.reshape(IMG, LOCAL, PATCH).transpose(0, 2, 1), dwin, dwout, db, dgain, dshift


def solution(mesh):
    placed = (P("dp", None, "chan"), P("dp", None, "chan"), P(), P(), P(), P(), P())
    return jax.shard_map(
        shards,
        mesh=mesh,
        in_specs=placed,
        out_specs=(P("dp", None, "chan"), P(), P(), P(), P("chan"), P("chan")),
        check_vma=False,
    )
```

```python
import math

import jax
import jax.numpy as jnp
from jax import lax
from jax.experimental import pallas as pl
from jax.experimental.pallas import tpu as pltpu
from jax.sharding import PartitionSpec as P

CHANNELS = 1280
PATCH = 256
HID = 640
LOCAL = 160
IMG = 8
ROWS = IMG * LOCAL
IMAGES = 256
MESH = pl.DeviceIdType.MESH
PIECES = ((0, 384, False), (384, 256, True))
PARTS = {False: 16, True: 10}
eps_norm = 1e-05
F32, BF16 = jnp.float32, jnp.bfloat16


def remote(src, dst, send, recv, dev):
    return pltpu.make_async_remote_copy(
        src_ref=src, dst_ref=dst, send_sem=send, recv_sem=recv, device_id=dev, device_id_type=MESH
    )


def arrived(ref, sem):
    pltpu.make_async_copy(ref, ref, sem).wait()


def each(n, body):
    def step(i, carry):
        body(i)
        return carry

    lax.fori_loop(0, n, step, 0)


def div(a, b):
    return lax.div(jnp.int32(a), jnp.int32(b))


def rem(a, b):
    return lax.rem(jnp.int32(a), jnp.int32(b))


def place():
    dp, ch = lax.axis_index("dp"), lax.axis_index("chan")
    x, zl, y = div(dp, 8), rem(div(dp, 4), 2), rem(dp, 4)
    zh, core = div(ch, 2), rem(ch, 2)
    return x, y, zh * 2 + zl, core


def device(x, y, z, core):
    return (x * 8 + rem(z, 2) * 4 + y, div(z, 2) * 2 + core)


def dot(a, b):
    return jnp.dot(a, b, preferred_element_type=F32)


def dot_nt(a, b):
    return lax.dot_general(a, b, (((1,), (1,)), ((), ())), preferred_element_type=F32)


def slot(which, image):
    return image // 4 * 8 + which * 4 + image % 4


def kernel(
    x_hbm, g_hbm, win_hbm, wout_hbm, b_hbm, gain_hbm, bias_hbm,
    out_ref, *refs,
):
    fulls, (sum_ref, *refs) = refs[: len(PIECES)], refs[len(PIECES) :]
    travel = refs[41:]
    (
        xv, win, wout, winT, bv, gain_v, bias_v, rows5, rows10, left, flip, right, ga, xh, rs, gn, gcol,
        e_src, e_far, f_src, f_in, f_sum, f_far,
        small, sm1, smt, sm2, sm3, sm4,
        ld, es, eq, fs, fq1, fq2, a1, b1, a2, b2, a3, b3,
    ) = refs[:41]
    x, y, z, core = place()
    other = 1 - core
    q = x * 4 + y
    partner = device(x, y, z, other)
    sends = []
    pieces = []
    for (at, width, direct), full in zip(PIECES, fulls):
        n = PARTS[direct]
        pieces.append((pl.ds(at, width), direct, full, travel[:n]))
        travel = travel[n:]

    def start(c):
        c.start()
        sends.append(c)

    def plane(j, c=core):
        xx, yy = rem(x + div(j, 4), 4), rem(y + rem(j, 4), 4)
        return device(xx, yy, z, c), xx * 4 + yy

    def column(d, c=core):
        return device(x, y, rem(z + d, 8), c)

    def image(b):
        return pl.ds(b * LOCAL, LOCAL)

    loads = [
        pltpu.make_async_copy(a, b, ld.at[i])
        for i, (a, b) in enumerate(
            (
                (g_hbm, left.at[1]), (wout_hbm, wout), (win_hbm, win),
                (b_hbm, bv), (gain_hbm, gain_v), (bias_hbm, bias_v),
            )
        )
    ]
    def chan_peers():
        return [column(d, c) for d in (4, 2, 6) for c in (core, other)] + [partner]

    def hop(i):
        return 1 + rem(3 + i, 7)

    def offset(i):
        return 1 + rem(9 + i, 15)

    barrier = pltpu.get_barrier_semaphore()

    def greet(dev):
        pl.semaphore_signal(barrier, inc=1, device_id=dev, device_id_type=MESH)

    for dev in chan_peers():
        greet(dev)
    for d in (3, 5, 1, 7):
        greet(column(d))
    each(15, lambda i: greet(plane(offset(i))[0]))

    x_loads = [
        pltpu.make_async_copy(x_hbm.at[image(b)], xv.at[image(b)], ld.at[8 + b]) for b in range(IMG)
    ]
    for c in x_loads + loads:
        c.start()

    for b in range(IMG):
        x_loads[b].wait()
        v = xv[image(b), :].astype(F32)
        e_src[b // 4, pl.ds(b % 4, 1), :] = jnp.sum(v, axis=0, keepdims=True)
        e_src[b // 4, pl.ds(4 + b % 4, 1), :] = jnp.sum(v * v, axis=0, keepdims=True)
    pl.semaphore_wait(barrier, 26)
    for h in range(2):
        for n, dev in enumerate(chan_peers()):
            start(remote(e_src.at[h], e_far.at[h, n], es.at[7 * h + n], eq.at[h], dev))

    def second_step(src, came, summed, far, sem1, send, sem2):
        arrived(came, sem1)
        both = src[...] + came[...]
        summed[0] = both[:8]
        summed[1] = both[8:]
        n = 1
        for d in (4, 2, 6):
            for c in (core, other):
                start(remote(summed.at[core], far.at[d // 2 - 1, core], send.at[n], sem2, column(d, c)))
                n += 1

    def finish(summed, far, sem2):
        arrived(far, sem2)
        tot = (summed[...] + far[0] + far[1] + far[2]) * (1.0 / CHANNELS)
        return lambda which, b: tot[b // 4, which * 4 + b % 4 : which * 4 + b % 4 + 1, :]

    for c in loads:
        c.wait()
    where = div(z, 2) * 2 + core
    for i in range(2):
        rows10[...] = (gain_v, bias_v)[i][...].reshape(10, 128)
        at = div(where * 5, 4)
        both = jnp.concatenate([rows10[pl.ds(at, 1), :], rows10[pl.ds(at + 1, 1), :]], axis=1)
        mine = pltpu.roll(both, rem(256 - rem(where * 5, 4) * 32, 256), 1)
        col = jnp.transpose(jnp.broadcast_to(mine, (128, 256)))
        gcol[i] = jnp.broadcast_to(col[:LOCAL, 0:1], (LOCAL, PATCH))
    winT[...] = jnp.transpose(win[...])
    for b in range(IMG):
        ga[image(b), :] = dot(left[1, image(b), :], wout[...])
    flip[1] = jnp.transpose(left[1])

    rows5[...] = bv[...].reshape(5, 128)
    bias = jnp.concatenate([rows5[i : i + 1, :] for i in range(5)], axis=1)

    def hidden(b, at, width):
        ks = pl.ds(at, width)
        pre = dot(left[0, image(b), :], winT[:, ks]) + bias[:, at : at + width]
        cdf = 0.5 * (1.0 + lax.erf(pre * (1.0 / math.sqrt(2.0))))
        right[1, image(b), ks] = (pre * cdf).astype(BF16)
        slope = cdf + pre * jnp.exp(-0.5 * pre * pre) * (1.0 / math.sqrt(2.0 * math.pi))
        right[0, image(b), ks] = (ga[image(b), ks] * slope).astype(BF16)

    for h in range(2):
        arrived(e_far.at[h], eq.at[h])
        tot = e_src[h]
        for n in range(7):
            tot = tot + e_far[h, n]
        tot = tot * (1.0 / CHANNELS)
        means = tot[:4]
        rstd = lax.rsqrt(tot[4:] - means * means + eps_norm)
        rs[pl.ds(4 * h, 4), :] = rstd
        for i in range(4):
            b = 4 * h + i
            xhat = (xv[image(b), :].astype(F32) - means[i : i + 1, :]) * rstd[i : i + 1, :]
            xh[image(b), :] = xhat
            left[0, image(b), :] = (xhat * gcol[0] + gcol[1]).astype(BF16)
            hidden(b, *PIECES[0][:2])
    flip[0] = jnp.transpose(left[0])

    def scatter(direct, parts):
        if direct:
            grads, r1, _, _, s1, q1, *_ = parts

            def give(i):
                j = rem(10 + i, 16)
                dev, qq = plane(j, other)
                remote(grads.at[other, qq], r1.at[16 + j], s1, q1, dev).start()

            def give_own(i):
                dev, qq = plane(offset(i))
                remote(grads.at[core, qq], r1.at[offset(i)], s1, q1, dev).start()
                give(i)

            each(15, give_own)
            give(15)
            return
        grads, r0, s, r1, _, _, _, q0, s1, q1, *_ = parts
        arrived(r0, q0)

        def add(i):
            s[i] = (grads[core, i].astype(F32) + r0[i].astype(F32)).astype(BF16)

        each(16, add)

        def give(i):
            dev, qq = plane(offset(i))
            remote(s.at[qq], r1.at[offset(i)], s1, q1, dev).start()

        each(15, give)

    waiting = None
    for (at, width, _), (ks, direct, _, parts) in zip(PIECES, pieces):
        if at:
            for b in range(IMG):
                hidden(b, at, width)
        if waiting:
            scatter(*waiting)
        grads = parts[0]
        grads[other] = dot(flip[other], right[other, :, ks]).astype(BF16).reshape(16, 16, width)
        if not direct:
            start(remote(grads.at[other], parts[1], parts[6], parts[7], partner))
        grads[core] = dot(flip[core], right[core, :, ks]).astype(BF16).reshape(16, 16, width)
        waiting = direct, parts
    scatter(*waiting)

    by_gain = by_shift = None
    for b in range(IMG):
        v = dot(right[0, image(b), :], win[...]).astype(BF16)
        gn[image(b), :] = v
        v = v.astype(F32)
        along = v * xh[image(b), :]
        f_src[pl.ds(slot(0, b), 1), :] = jnp.sum(v * gcol[0], axis=0, keepdims=True)
        f_src[pl.ds(slot(1, b), 1), :] = jnp.sum(along * gcol[0], axis=0, keepdims=True)
        by_gain = along if b == 0 else by_gain + along
        by_shift = v if b == 0 else by_shift + v
    start(remote(f_src, f_in, fs.at[0], fq1, partner))

    db = dot(jnp.ones((8, ROWS), BF16), right[0])[0:1]
    for i in range(5):
        small[pl.ds(i, 1), :] = db[:, i * 128 : i * 128 + 128]
    ones = jnp.ones((8, PATCH), BF16)
    for i, v in enumerate((by_gain, by_shift)):
        hi = v.astype(BF16)
        rest = v - hi.astype(F32)
        mid = rest.astype(BF16)
        low = (rest - mid.astype(F32)).astype(BF16)
        one = (dot_nt(ones, hi) + dot_nt(ones, mid) + dot_nt(ones, low))[0:1]
        small[pl.ds(5 + i, 1), :] = one[:, :128]
        small[pl.ds(7, 1), pl.ds(32 * i, 32)] = one[:, 128:]
    small[pl.ds(7, 1), pl.ds(64, 64)] = jnp.zeros((1, 64), F32)
    each(15, lambda i: remote(small, sm1.at[offset(i)], a1, b1, plane(offset(i))[0]).start())

    second_step(f_src, f_in, f_sum, f_far, fq1, fs, fq2)

    for _, direct, _, parts in pieces:
        if direct:
            grads, r1, t, r2, _, q1, s2, q2, *_ = parts
            arrived(r1.at[pl.ds(1, 31)], q1)
            acc = grads[core, q].astype(F32)
        else:
            _, _, s, r1, t, r2, _, _, _, q1, s2, q2, *_ = parts
            arrived(r1.at[pl.ds(1, 15)], q1)
            acc = s[q].astype(F32)
        t[...] = lax.fori_loop(1, r1.shape[0], lambda j, a: a + r1[j].astype(F32), acc, unroll=r1.shape[0] - 1).astype(BF16)
        each(7, lambda i: remote(t, r2.at[hop(i)], s2, q2, column(hop(i))).start())

    moment = finish(f_sum, f_far, fq2)
    for b in range(IMG):
        inner = gn[image(b), :].astype(F32) * gcol[0] - moment(0, b) - xh[image(b), :] * moment(1, b)
        out_ref[image(b), :] = (left[1, image(b), :].astype(F32) + rs[pl.ds(b, 1), :] * inner).astype(BF16)

    for _, direct, full, parts in pieces:
        t, r2, s2, q2, s3, q3 = parts[2:4] + parts[6:] if direct else parts[4:6] + parts[10:14]
        arrived(r2.at[pl.ds(1, 7)], q2)
        acc = lax.fori_loop(1, 8, lambda d, a: a + r2[d].astype(F32), t[...].astype(F32), unroll=7)
        full[core, q] = acc.astype(BF16)
        mine = full.at[core, q]

        def tell(i):
            remote(mine, mine, s3, q3, plane(offset(i))[0]).start()
            if direct:
                remote(mine, mine, s3, q3, plane(offset(i), other)[0]).start()

        each(15, tell)
        if direct:
            remote(mine, mine, s3, q3, partner).start()
        else:
            arrived(sm1.at[pl.ds(1, 15)], b1)
            smt[...] = lax.fori_loop(1, 16, lambda j, a: a + sm1[j], small[...])
            each(7, lambda i: remote(smt, sm2.at[hop(i)], a2, b2, column(hop(i))).start())

    arrived(sm2.at[pl.ds(1, 7)], b2)
    near = smt[...] + sm2[7 - 6 * rem(z, 2)]
    sm3[...] = lax.fori_loop(1, 8, lambda d, a: a + sm2[d], smt[...])
    start(remote(sm3, sm4, a3, b3, partner))
    for _, direct, full, parts in pieces:
        if not direct:
            q3, s4, q4 = parts[13:]
            arrived(full.at[core, pl.ds(1, 15)], q3)
            remote(full.at[core], full.at[core], s4, q4, partner).start()
    arrived(sm4, b3)
    row = lax.broadcasted_iota(jnp.int32, (8, 128), 0)
    sum_ref[...] = jnp.where(row < 5, sm3[...] + sm4[...], near) * (1.0 / IMAGES)
    for _, direct, full, parts in pieces:
        if direct:
            grads, r1, t, r2, s1, q1, s2, q2, s3, q3 = parts
            r1 = r1.at[pl.ds(1, 31)]
            arrived(r1, q3)
            arrived(r1, s3)
        else:
            _, _, _, r1, _, r2, _, _, s1, _, s2, _, s3, _, s4, q4 = parts
            r1 = r1.at[pl.ds(1, 15)]
            arrived(full.at[other], q4)
            arrived(r1, s3)
            arrived(full.at[core], s4)
        arrived(r1, s1)
        arrived(r2.at[pl.ds(1, 7)], s2)
    arrived(sm1.at[pl.ds(1, 15)], a1)
    arrived(sm2.at[pl.ds(1, 7)], a2)
    for c in sends:
        c.wait_send()


def last_kernel(d_ref, *refs):
    fulls, refs = refs[: len(PIECES)], refs[len(PIECES) :]
    sum_ref, out, dwin, dwout, db, gain, shift, v1, v2, v3, v4, v5, sem = refs
    copies = []

    def put(i, src, dst):
        c = pltpu.make_async_copy(src, dst, sem.at[i])
        c.start()
        copies.append(c)

    put(0, d_ref, out)
    for (at, width, _), full in zip(PIECES, fulls):
        v2[:, pl.ds(at, width)] = full[1].reshape(PATCH, width).astype(F32) * (1.0 / IMAGES)
    put(1, v2, dwout)
    for n, ((at, width, _), full) in enumerate(zip(PIECES, fulls)):
        rows = pl.ds(at, width)
        v1[rows, :] = jnp.transpose(full[0].reshape(PATCH, width).astype(F32)) * (1.0 / IMAGES)
        put(6 + n, v1.at[rows], dwin.at[rows])
    v3[...] = sum_ref[0:5, :].reshape(HID)
    put(3, v3, db)
    for i, (v, dst) in enumerate(((v4, gain), (v5, shift))):
        v[pl.ds(0, 128)] = sum_ref[5 + i, :]
        v[pl.ds(128, 32)] = sum_ref[7, 32 * i : 32 * i + 32]
        put(4 + i, v, dst)
    for c in copies:
        c.wait()


def buf(dtype, *shape):
    return pltpu.VMEM(shape, dtype)


def shards(patches, cotangent, w_in, b_in, w_out, gain, bias):
    dma = pltpu.SemaphoreType.DMA
    vmem = pl.BlockSpec(memory_space=pltpu.VMEM)
    hbm = pl.BlockSpec(memory_space=pltpu.HBM)

    def turned(v):
        return v.transpose(0, 2, 1).reshape(ROWS, PATCH)

    def piece(width, direct):
        halves = [buf(BF16, 16, 16, width), buf(BF16, 16, 16, width)]
        return [
            buf(BF16, 2, 16, 16, width),
            *([] if direct else halves),
            buf(BF16, 32 if direct else 16, 16, width),
            buf(BF16, 16, width),
            buf(BF16, 8, 16, width),
            *[dma] * (6 if direct else 10),
        ]

    d, *fulls, sums = pl.pallas_call(
        kernel,
        out_shape=(
            jax.ShapeDtypeStruct((ROWS, PATCH), BF16),
            *(jax.ShapeDtypeStruct((2, 16, 16, width), BF16) for _, width, _ in PIECES),
            jax.ShapeDtypeStruct((8, 128), F32),
        ),
        in_specs=[hbm] * 7,
        out_specs=(vmem,) * (2 + len(PIECES)),
        scratch_shapes=[
            buf(BF16, ROWS, PATCH),
            buf(BF16, HID, PATCH),
            buf(BF16, PATCH, HID),
            buf(BF16, PATCH, HID),
            buf(F32, HID),
            buf(F32, CHANNELS),
            buf(F32, CHANNELS),
            buf(F32, 5, 128),
            buf(F32, 10, 128),
            buf(BF16, 2, ROWS, PATCH),
            buf(BF16, 2, PATCH, ROWS),
            buf(BF16, 2, ROWS, HID),
            buf(F32, ROWS, HID),
            buf(F32, ROWS, PATCH),
            buf(F32, 8, PATCH),
            buf(BF16, ROWS, PATCH),
            buf(F32, 2, LOCAL, PATCH),
            buf(F32, 2, 8, PATCH), buf(F32, 2, 7, 8, PATCH),
            buf(F32, 16, PATCH), buf(F32, 16, PATCH), buf(F32, 2, 8, PATCH), buf(F32, 3, 2, 8, PATCH),
            buf(F32, 8, 128),
            buf(F32, 16, 8, 128), buf(F32, 8, 128), buf(F32, 8, 8, 128), buf(F32, 8, 128), buf(F32, 8, 128),
            dma((16,)), dma((14,)), dma((2,)), dma((7,)), dma, dma,
            dma, dma, dma, dma, dma, dma,
            *(v for _, width, direct in PIECES for v in piece(width, direct)),
        ],
        compiler_params=pltpu.CompilerParams(collective_id=0, has_side_effects=True, vmem_limit_bytes=40000000),
    )(
        *(
            pltpu.with_memory_space_constraint(v, pltpu.HBM)
            for v in (turned(patches), turned(cotangent), w_in, w_out, b_in, gain, bias)
        )
    )
    out, dwin, dwout, db, dgain, dshift = pl.pallas_call(
        last_kernel,
        out_shape=(
            jax.ShapeDtypeStruct((ROWS, PATCH), BF16),
            jax.ShapeDtypeStruct((HID, PATCH), F32),
            jax.ShapeDtypeStruct((PATCH, HID), F32),
            jax.ShapeDtypeStruct((HID,), F32),
            jax.ShapeDtypeStruct((LOCAL,), F32),
            jax.ShapeDtypeStruct((LOCAL,), F32),
        ),
        in_specs=[vmem] * (2 + len(PIECES)),
        out_specs=(hbm,) * 6,
        scratch_shapes=[
            buf(F32, HID, PATCH), buf(F32, PATCH, HID), buf(F32, HID), buf(F32, LOCAL), buf(F32, LOCAL), dma((6 + len(PIECES),)),
        ],
        compiler_params=pltpu.CompilerParams(vmem_limit_bytes=8 * 1024 * 1024),
    )(d, *fulls, sums)
    return out.reshape(IMG, LOCAL, PATCH).transpose(0, 2, 1), dwin, dwout, db, dgain, dshift


def solution(mesh):
    placed = (P("dp", None, "chan"), P("dp", None, "chan"), P(), P(), P(), P(), P())
    return jax.shard_map(
        shards,
        mesh=mesh,
        in_specs=placed,
        out_specs=(P("dp", None, "chan"), P(), P(), P(), P("chan"), P("chan")),
        check_vma=False,
    )
```
